32 devices in a mesh: replica: 8 (over z, y), tensor: 4 (over x, core).
Axes of the slice: x: 2, y: 2, z: 4, core: 2. Of those that a mesh axis runs over, the one named last changes fastest.
Arguments:
- activations: bfloat16 [8192, 2048], P('replica', 'tensor'), may hold values from -0.625 to 0.625
- grad_out: bfloat16 [8192, 7168], P('replica', 'tensor'), may hold values from -6 to 6
- weight: bfloat16 [2048, 7168], P(None, 'tensor'), may hold values from -0.0625 to 0.0625
- momentum: float32 [8, 2048, 7168], P('replica', None, 'tensor'), may hold values from -6 to 6
- freq_rows: int32 [8, 32, 112], P(None, None, 'tensor'), may hold values from 0 to 63
Outputs:
- input_grad: bfloat16 [8192, 2048], P('replica', 'tensor')
- momentum_out: float32 [8, 2048, 7168], P('replica', None, 'tensor')
- update: bfloat16 [2048, 7168], P(None, 'tensor')
The draws below stay inside these ranges and needn't reach their ends.
All inputs are finite; a program needn't handle non-finite values.
Results may differ from the reference program's by a relative error of at most 0.001.
Values may be sent and summed in bfloat16 or wider, within the bound.
No kernel may reach another device: no remote copies, remote signals or barrier semaphores. Data moves between devices by JAX's collectives and lax.ppermute only.
A program may use at most 192 MiB of HBM per device.

```python
import jax
import jax.numpy as jnp
from jax import lax

D = 2048
FF = 7168
TILE = 64
TOK_DEV = 1024
TOKENS = 8192
TILE_ROWS = 32
TILE_COLS = 112
N_REPLICA = 8


def touch_ends(entries, stream_key, smallest, largest):
    longest = entries.shape.index(max(entries.shape))
    spots = []
    for shift in (0, 1):
        where = [jax.random.randint(jax.random.fold_in(stream_key, axis), (), 0, length) for axis, length in enumerate(entries.shape)]
        where[longest] = (where[longest] + shift) % entries.shape[longest]
        spots.append(tuple(where))
    return entries.at[spots[0]].set(smallest).at[spots[1]].set(largest)


def level_of(rng, extent, cuts, smallest, largest):
    loudness = 1.0
    for axis_at, blocks in cuts:
        steps = jax.random.uniform(jax.random.fold_in(jax.random.fold_in(rng, 6), axis_at), (blocks,), jnp.float32, smallest / len(cuts), largest / len(cuts))
        loudness = loudness * jnp.repeat(jnp.exp(steps), extent[axis_at] // blocks).reshape((-1,) + (1,) * (len(extent) - 1 - axis_at))
    return loudness


def scatter_about(key, shape, deviation, reach, cuts=(), kind=jnp.bfloat16):
    values = deviation * jax.random.normal(key, shape, jnp.float32)
    if cuts:
        values = values * level_of(key, shape, cuts, -0.22, 0.18)
    return jnp.clip(values, -reach, reach).astype(kind)


def setup_inputs(seed: int = 0) -> dict:
    splits = jax.random.split(jax.random.key(seed), 6)
    return {
        "activations": scatter_about(splits[0], (TOKENS, D), 0.04, 0.625, ((0, 8), (1, 4))),
        "grad_out": scatter_about(splits[1], (TOKENS, FF), 1.0, 6.0, ((0, 8), (1, 4))),
        "weight": scatter_about(splits[2], (D, FF), FF ** -0.5, 0.0625, ((1, 4),)),
        "momentum": scatter_about(splits[3], (N_REPLICA, D, FF), 1.0, 6.0, ((0, 8), (2, 4)), jnp.float32),
        "freq_rows": touch_ends(jax.random.randint(splits[4], (N_REPLICA, TILE_ROWS, TILE_COLS), 0, TILE), jax.random.fold_in(splits[4], 1), 0, TILE - 1).astype(jnp.int32),
    }


decay_rate = 0.9
highest = lax.Precision.HIGHEST

def cosine_table():
    freq = jnp.arange(TILE, dtype=jnp.float32)[:, None]
    place = jnp.arange(TILE, dtype=jnp.float32)[None, :]
    values = jnp.cos(jnp.pi * (2.0 * place + 1.0) * freq / (2.0 * TILE)) * jnp.sqrt(2.0 / TILE)
    return jnp.where(freq == 0.0, values / jnp.sqrt(2.0), values)

def one_replica(inputs):
    acts, grads, moment, chosen = inputs
    basis = cosine_table()
    weight_grad = jnp.dot(acts.T, grads, preferred_element_type=jnp.float32)
    kept = decay_rate * moment + weight_grad
    tile_view = kept.reshape(TILE_ROWS, TILE, TILE_COLS, TILE)
    half_done = jnp.einsum('ancm,lm->ancl', tile_view, basis, precision=highest)
    onehot = (chosen[:, :, None] == jnp.arange(TILE, dtype=jnp.int32)[None, None, :]).astype(jnp.float32)
    picked = jnp.einsum('ack,kn->acn', onehot, basis, precision=highest)
    coeff_rows = jnp.einsum('acn,ancl->acl', picked, half_done, precision=highest)
    spread = jnp.einsum('acj,jm->acm', coeff_rows, basis, precision=highest)
    removed = jnp.einsum('acn,acm->ancm', picked, spread)
    return (kept - removed.reshape(D, FF), coeff_rows)

def reference(activations, grad_out, weight, momentum, freq_rows):
    basis = cosine_table()
    input_grad = lax.dot_general(grad_out, weight, (((1,), (1,)), ((), ())), preferred_element_type=jnp.float32).astype(jnp.bfloat16)
    acts = activations.reshape(N_REPLICA, TOK_DEV, D)
    grads = grad_out.reshape(N_REPLICA, TOK_DEV, FF)
    momentum_out, coeff_all = lax.map(one_replica, (acts, grads, momentum, freq_rows))
    onehot = (freq_rows[..., None] == jnp.arange(TILE, dtype=jnp.int32)).astype(jnp.float32)
    summed = jnp.einsum('rack,racj->ackj', onehot, coeff_all, precision=highest)
    right_done = jnp.einsum('ackj,jm->ackm', summed, basis, precision=highest)
    decoded = jnp.einsum('kn,ackm->ancm', basis, right_done, precision=highest)
    update = decoded.reshape(D, FF).astype(jnp.bfloat16)
    return (input_grad, momentum_out, update)
```

```python
import functools

import jax
import jax.numpy as jnp
import numpy as np
from jax import lax
from jax.experimental import pallas as pl
from jax.experimental.pallas import tpu as pltpu
from jax.sharding import PartitionSpec as P


TILE = 64
LANES = 128
STEP = 256
PER_STEP = STEP // TILE
PAD = 8

MIB = 1 << 20


decay_rate = 0.9
highest = lax.Precision.HIGHEST


def cosine_table():
    freq = jnp.arange(TILE, dtype=jnp.float32)[:, None]
    place = jnp.arange(TILE, dtype=jnp.float32)[None, :]
    values = jnp.cos(jnp.pi * (2.0 * place + 1.0) * freq / (2.0 * TILE)) * jnp.sqrt(2.0 / TILE)
    return jnp.where(freq == 0.0, values / jnp.sqrt(2.0), values)


def cosine_constant():
    freq = np.arange(TILE)[:, None]
    place = np.arange(TILE)[None, :]
    values = np.cos(np.pi * (2 * place + 1) * freq / (2 * TILE)) * np.sqrt(2 / TILE)
    return np.where(freq == 0, values / np.sqrt(2), values).astype(np.float32)


def split3(values):
    first = values.astype(jnp.bfloat16)
    rest = values - first.astype(np.float32)
    second = rest.astype(jnp.bfloat16)
    third = (rest - second.astype(np.float32)).astype(jnp.bfloat16)
    return first, second, third


def encode(values):
    largest = jnp.maximum(jnp.max(jnp.abs(values), axis=0, keepdims=True), 1e-30)
    power = jnp.ceil(jnp.log2(largest * (1.0 / 32767.0)))
    whole = jnp.clip(jnp.round(values * jnp.exp2(-power)), -32767.0, 32767.0)
    return whole, power


def decode_block(whole, power):
    return whole * jnp.exp2(power)


def block_of(ids_ref, place, per_owner):
    return (ids_ref[0] ^ place[0]) * per_owner + place[1]


def grad_kernel(pieces, places, per_owner, chained, *refs):
    refs = list(refs)
    ids_ref, chosen_ref = refs[:2]
    acts_refs, refs = refs[2 : 2 + pieces], refs[2 + pieces :]
    go_ref, mom_ref, ct_ref = refs[:3]
    refs = refs[4:] if chained else refs[3:]
    out_ref, code_ref = refs[:2]
    go_buf, acts_buf, mom_buf, g_ref, tab_ref, rows_ref, in_sem, out_sem = refs[2:]
    steps = len(places)
    _, hidden = go_buf.shape

    def rows_of(step):
        start = block_of(ids_ref, places[step], per_owner) * STEP
        return pl.ds(pl.multiple_of(start, STEP), STEP)

    go_copy = pltpu.make_async_copy(go_ref, go_buf, in_sem.at[2 * steps])
    go_copy.start()
    step = 0
    for piece in acts_refs:
        for n in range(piece.shape[1] // STEP):
            source = piece.at[:, pl.ds(n * STEP, STEP)]
            pltpu.make_async_copy(source, acts_buf.at[step], in_sem.at[step]).start()
            source = mom_ref.at[rows_of(step), :]
            pltpu.make_async_copy(source, mom_buf.at[step], in_sem.at[steps + step]).start()
            step += 1
    for k in range(TILE):
        tab_ref[k] = jnp.broadcast_to(ct_ref[:, k : k + 1], (TILE, LANES))
    left = lax.broadcasted_iota(jnp.int32, (TILE, LANES), 1) < TILE
    go_copy.wait()
    for step in range(steps):
        here = acts_buf.at[step]
        pltpu.make_async_copy(here, here, in_sem.at[step]).wait()
        g_ref[...] = lax.dot_general(
            acts_buf[step], go_buf[...], (((0,), (0,)), ((), ())), preferred_element_type=jnp.float32
        )
        here = mom_buf.at[step]
        pltpu.make_async_copy(here, here, in_sem.at[steps + step]).wait()
        block = block_of(ids_ref, places[step], per_owner)

        def tile_row(tr, carry):
            rows = pl.ds(pl.multiple_of(tr * TILE, TILE), TILE)
            tile = block * PER_STEP + tr
            for pair in range(hidden // LANES):
                lanes = pl.ds(pair * LANES, LANES)
                picked = jnp.where(
                    left,
                    tab_ref[chosen_ref[tile, 2 * pair]],
                    tab_ref[chosen_ref[tile, 2 * pair + 1]],
                )
                kept = decay_rate * mom_buf[step, rows, lanes] + g_ref[rows, lanes]
                row = jnp.sum(kept * picked, axis=0, keepdims=True)
                mom_buf[step, rows, lanes] = kept - picked * row
                rows_ref[step * PER_STEP + tr, :, lanes] = row
            return carry

        lax.fori_loop(0, PER_STEP, tile_row, 0)
        pltpu.make_async_copy(mom_buf.at[step], out_ref.at[rows_of(step), :], out_sem.at[step]).start()
    whole, power = encode(jnp.concatenate([rows_ref[n] for n in range(steps * PER_STEP)], axis=0))
    power = jnp.broadcast_to(power, (PAD, power.shape[1]))
    code_ref[...] = jnp.concatenate([whole, power], axis=0).astype(jnp.int32).astype(jnp.int16)
    for step in range(steps):
        pltpu.make_async_copy(mom_buf.at[step], out_ref.at[rows_of(step), :], out_sem.at[step]).wait()


def grad_call(places, ids, chosen, acts, grad_out, momentum, per_owner, chained):
    tokens, hidden = grad_out.shape
    features = momentum.shape[0]
    steps = len(places)
    rows = steps * PER_STEP
    anywhere = pl.BlockSpec(memory_space=pl.ANY)
    operands = [ids, chosen, *acts, grad_out, momentum, cosine_constant().T.copy()]
    far = pl.BlockSpec(memory_space=pltpu.HBM)
    in_specs = [anywhere] * (len(acts) + 1) + [far]
    in_specs.append(pl.BlockSpec((TILE, TILE), lambda i, ids, cho: (0, 0)))
    aliases = {}
    if chained is not None:
        aliases = {len(operands): 0}
        operands.append(chained)
        in_specs.append(far)
    return pl.pallas_call(
        functools.partial(grad_kernel, len(acts), places, per_owner, chained is not None),
        grid_spec=pltpu.PrefetchScalarGridSpec(
            num_scalar_prefetch=2,
            grid=(1,),
            in_specs=in_specs,
            out_specs=[far, pl.BlockSpec((rows + PAD, hidden), lambda i, ids, cho: (0, 0))],
            scratch_shapes=[
                pltpu.VMEM((tokens, hidden), grad_out.dtype),
                pltpu.VMEM((steps, tokens, STEP), grad_out.dtype),
                pltpu.VMEM((steps, STEP, hidden), jnp.float32),
                pltpu.VMEM((STEP, hidden), jnp.float32),
                pltpu.VMEM((TILE, TILE, LANES), jnp.float32),
                pltpu.VMEM((rows + PAD, 1, hidden), jnp.float32),
                pltpu.SemaphoreType.DMA((2 * steps + 1,)),
                pltpu.SemaphoreType.DMA((steps,)),
            ],
        ),
        out_shape=[
            jax.ShapeDtypeStruct((features, hidden), jnp.float32),
            jax.ShapeDtypeStruct((rows + PAD, hidden), jnp.int16),
        ],
        input_output_aliases=aliases,
        cost_estimate=pl.CostEstimate(
            flops=2 * steps * STEP * tokens * hidden,
            bytes_accessed=2 * tokens * hidden + 8 * steps * STEP * hidden,
            transcendentals=0,
        ),
        compiler_params=pltpu.CompilerParams(
            vmem_limit_bytes=50 * MIB
        ),
        name="grad_step",
    )(*operands)


def partial_kernel(masks, ids_ref, go_ref, w_ref, *refs):
    out_refs, (go_buf, w_buf, out_buf, in_sem, out_sem) = refs[: len(masks)], refs[len(masks) :]
    chunks, rows, _ = go_buf.shape
    width = w_buf.shape[1]
    copies = []
    for n, mask in enumerate(masks):
        start = pl.multiple_of((ids_ref[0] ^ mask) * width, width)
        copies.append(pltpu.make_async_copy(w_ref.at[pl.ds(start, width), :], w_buf.at[n], in_sem.at[n]))
    for n in range(chunks):
        source = go_ref.at[pl.ds(n * rows, rows), :]
        copies.append(pltpu.make_async_copy(source, go_buf.at[n], in_sem.at[len(masks) + n]))
    for n in (0, len(masks), *range(1, len(masks)), *range(len(masks) + 1, len(copies))):
        copies[n].start()
    outs = []
    for n in range(chunks):
        copies[len(masks) + n].wait()
        for m in range(len(masks)):
            if n == 0:
                copies[m].wait()
            out_buf[m, n] = lax.dot_general(
                go_buf[n], w_buf[m], (((1,), (1,)), ((), ())), preferred_element_type=jnp.float32
            )
            target = out_refs[m].at[pl.ds(n * rows, rows), :]
            outs.append(pltpu.make_async_copy(out_buf.at[m, n], target, out_sem.at[m, n]))
            outs[-1].start()
    for copy in outs:
        copy.wait()


def partial_call(masks, ids, grad_out, weight, width):
    tokens, hidden = grad_out.shape
    chunks = 2
    rows = tokens // chunks
    shape = jax.ShapeDtypeStruct((tokens, width), jnp.float32)
    anywhere = pl.BlockSpec(memory_space=pl.ANY)
    return pl.pallas_call(
        functools.partial(partial_kernel, masks),
        grid_spec=pltpu.PrefetchScalarGridSpec(
            num_scalar_prefetch=1,
            grid=(1,),
            in_specs=[anywhere, pl.BlockSpec(memory_space=pltpu.HBM)],
            out_specs=[anywhere] * len(masks),
            scratch_shapes=[
                pltpu.VMEM((chunks, rows, hidden), grad_out.dtype),
                pltpu.VMEM((len(masks), width, hidden), weight.dtype),
                pltpu.VMEM((len(masks), chunks, rows, width), jnp.float32),
                pltpu.SemaphoreType.DMA((len(masks) + chunks,)),
                pltpu.SemaphoreType.DMA((len(masks), chunks)),
            ],
        ),
        out_shape=[shape] * len(masks),
        cost_estimate=pl.CostEstimate(
            flops=2 * len(masks) * tokens * width * hidden,
            bytes_accessed=2 * tokens * hidden + len(masks) * width * (2 * hidden + 4 * tokens),
            transcendentals=0,
        ),
        compiler_params=pltpu.CompilerParams(
            vmem_limit_bytes=57 * MIB
        ),
        name="partial_products",
    )(ids, grad_out, weight)


def add_encode_kernel(a_ref, b_ref, out_ref):
    whole, power = encode(a_ref[...] + b_ref[...])
    power = jnp.broadcast_to(power, (2 * PAD, power.shape[1]))
    rows = whole.shape[0]
    out_ref[:rows, :] = whole.astype(jnp.int32).astype(jnp.int16)
    out_ref[rows:, :] = power.astype(jnp.int32).astype(jnp.int16)


def add_encode(a, b, blocks):
    tokens, width = a.shape
    rows = tokens // blocks
    spec = pl.BlockSpec((rows, width), lambda i: (i, 0))
    return pl.pallas_call(
        add_encode_kernel,
        grid=(blocks,),
        in_specs=[spec, spec],
        out_specs=pl.BlockSpec((rows + 2 * PAD, width), lambda i: (i, 0)),
        out_shape=jax.ShapeDtypeStruct((blocks * (rows + 2 * PAD), width), jnp.int16),
        cost_estimate=pl.CostEstimate(flops=8 * a.size, bytes_accessed=10 * a.size, transcendentals=0),
        compiler_params=pltpu.CompilerParams(vmem_limit_bytes=2 * MIB + 24 * rows * width),
        name="add_encode",
    )(a, b)


def add_decode_kernel(a_ref, b_ref, code_ref, out_ref):
    rows = a_ref.shape[0]
    whole = code_ref[:rows, :].astype(jnp.int32).astype(jnp.float32)
    power = code_ref[rows:, :].astype(jnp.int32).astype(jnp.float32)[:1]
    out_ref[...] = (a_ref[...] + b_ref[...] + decode_block(whole, power)).astype(out_ref.dtype)


def add_decode(a, b, code, blocks):
    tokens, width = a.shape
    rows = tokens // blocks
    spec = pl.BlockSpec((rows, width), lambda i: (i, 0))
    return pl.pallas_call(
        add_decode_kernel,
        grid=(blocks,),
        in_specs=[spec, spec, pl.BlockSpec((rows + 2 * PAD, width), lambda i: (i, 0))],
        out_specs=spec,
        out_shape=jax.ShapeDtypeStruct((tokens, width), jnp.bfloat16),
        cost_estimate=pl.CostEstimate(flops=8 * a.size, bytes_accessed=12 * a.size, transcendentals=0),
        compiler_params=pltpu.CompilerParams(vmem_limit_bytes=2 * MIB + 28 * rows * width),
        name="add_decode",
    )(a, b, code)


def update_kernel(places, per_owner, chained, ids_ref, near_ref, far_ref, freq_ref, ct_ref, *refs):
    if chained:
        refs = refs[1:]
    out_ref, held_ref, out_buf, out_sem = refs
    steps = len(places)
    rows = steps * PER_STEP
    hidden = out_ref.shape[1]
    total = near_ref.shape[0]
    replicas = 2 * total
    for side, ref in enumerate((near_ref, far_ref)):
        for slot in range(total):
            code = ref[slot].astype(jnp.int32).astype(jnp.float32)
            values = decode_block(code[:rows], code[rows : rows + 1])
            start = pl.multiple_of((ids_ref[1] ^ (2 * slot + side)) * rows, 8)
            for strip in range(hidden // LANES):
                held_ref[strip, pl.ds(start, rows), :] = values[:, strip * LANES : (strip + 1) * LANES]

    groups = hidden // (4 * TILE)
    wide = groups * LANES
    number = lax.broadcasted_iota(jnp.int32, (TILE, wide), 0)
    main = (lax.broadcasted_iota(jnp.int32, (TILE, wide), 1) % LANES) < TILE
    lane_tile = lax.broadcasted_iota(jnp.int32, (replicas, 4 * TILE), 1) // TILE

    for step in range(steps):
        block = block_of(ids_ref, places[step], per_owner)

        def tile_row(tr, carry):
            onehot = number == freq_ref[pl.ds(block * PER_STEP + tr, 1), :]
            onehot = onehot.astype(jnp.float32).astype(jnp.bfloat16)
            columns = jnp.dot(
                ct_ref[...],
                jnp.concatenate([onehot] * 3, axis=0),
                preferred_element_type=jnp.float32,
            )
            high = columns.astype(jnp.bfloat16).astype(jnp.float32)
            lhs = jnp.where(main, high, columns - high).astype(jnp.bfloat16)
            here = step * PER_STEP + tr
            row0 = pl.ds(pl.multiple_of(tr * TILE, TILE), TILE)
            for group in range(groups):
                values = jnp.concatenate(
                    [held_ref[2 * group + n, pl.ds(here, replicas, stride=rows), :] for n in range(2)],
                    axis=1,
                )
                top = values.astype(jnp.bfloat16).astype(jnp.float32)
                low = values - top
                parts = [jnp.where(lane_tile == c, part, 0.0) for part in (top, low) for c in range(4)]
                rhs = jnp.concatenate(parts, axis=0).astype(jnp.bfloat16)
                rhs = jnp.concatenate([rhs, rhs], axis=0)
                product = jnp.dot(
                    lhs[:, group * LANES : (group + 1) * LANES], rhs, preferred_element_type=jnp.float32
                )
                lanes = pl.ds(group * 4 * TILE, 4 * TILE)
                out_buf[step, row0, lanes] = product.astype(out_buf.dtype)
            return carry

        lax.fori_loop(0, PER_STEP, tile_row, 0, unroll=True)
        target = out_ref.at[pl.ds(pl.multiple_of(block * STEP, STEP), STEP), :]
        pltpu.make_async_copy(out_buf.at[step], target, out_sem.at[step]).start()
    for step in range(steps):
        block = block_of(ids_ref, places[step], per_owner)
        target = out_ref.at[pl.ds(pl.multiple_of(block * STEP, STEP), STEP), :]
        pltpu.make_async_copy(out_buf.at[step], target, out_sem.at[step]).wait()


def update_call(places, ids, near, far, freq_lanes, features, per_owner, chained):
    hidden = near.shape[2]
    steps = len(places)
    rows = steps * PER_STEP
    anywhere = pl.BlockSpec(memory_space=pltpu.HBM)
    table = jnp.concatenate(split3(cosine_constant().T), axis=1)
    operands = [ids, near, far, freq_lanes, table]
    in_specs = [
        pl.BlockSpec(near.shape, lambda i, ids: (0, 0, 0)),
        pl.BlockSpec(far.shape, lambda i, ids: (0, 0, 0)),
        pl.BlockSpec(freq_lanes.shape, lambda i, ids: (0, 0)),
        pl.BlockSpec(table.shape, lambda i, ids: (0, 0)),
    ]
    aliases = {}
    if chained is not None:
        aliases = {len(operands): 0}
        operands.append(chained)
        in_specs.append(anywhere)
    replicas = 2 * near.shape[0]
    return pl.pallas_call(
        functools.partial(update_kernel, places, per_owner, chained is not None),
        grid_spec=pltpu.PrefetchScalarGridSpec(
            num_scalar_prefetch=1,
            grid=(1,),
            in_specs=in_specs,
            out_specs=anywhere,
            scratch_shapes=[
                pltpu.VMEM((hidden // LANES, (replicas + 1) * rows, LANES), jnp.float32),
                pltpu.VMEM((steps, STEP, hidden), jnp.bfloat16),
                pltpu.SemaphoreType.DMA((steps,)),
            ],
        ),
        out_shape=jax.ShapeDtypeStruct((features, hidden), jnp.bfloat16),
        input_output_aliases=aliases,
        cost_estimate=pl.CostEstimate(
            flops=2 * rows * TILE * 512 * hidden, bytes_accessed=2 * rows * TILE * hidden, transcendentals=0
        ),
        compiler_params=pltpu.CompilerParams(
            vmem_limit_bytes=4 * MIB + 2 * rows * TILE * hidden + 4 * (replicas + 1) * rows * hidden + 4 * near.size * 4
        ),
        name="update_rows",
    )(*operands)


def flip(x, axis, mask):
    size = lax.axis_size(axis)
    return lax.ppermute(x, axis, [(i, i ^ mask) for i in range(size)])


def fast_body(activations, grad_out, weight, momentum, freq_rows):
    return fast_layer(activations, grad_out, weight, momentum, freq_rows)


def fast_layer(activations, grad_out, weight, momentum, freq_rows):
    device = lax.axis_index("tensor")
    replica = lax.axis_index("replica")
    ids = jnp.stack([device, replica])
    features, _ = weight.shape
    width = activations.shape[1]
    per_owner = width // STEP
    tile_rows, tile_cols = freq_rows.shape[1:]
    replicas = freq_rows.shape[0]

    chunks = [activations[:, n * STEP : (n + 1) * STEP] for n in range(per_owner)]
    twin = flip(activations, "tensor", 1)
    across = [flip(chunk, "tensor", 2) for chunk in chunks]
    across_twin = [flip(chunk, "tensor", 1) for chunk in across]

    for_twin, for_far = partial_call((3, 2), ids, grad_out, weight, width)
    received = flip(for_twin, "tensor", 1)
    code = add_encode(for_far, received, 2)
    code = flip(code, "tensor", 2)
    for_twin, own = partial_call((1, 0), ids, grad_out, weight, width)
    own_twin = flip(for_twin, "tensor", 1)

    chosen = lax.dynamic_index_in_dim(freq_rows, replica, 0, keepdims=False)
    kept = momentum[0]
    places = [
        tuple((mask, n) for mask in (0, 1) for n in range(per_owner)) + ((2, 0), (3, 0)),
    ] + [((2, n), (3, n)) for n in range(1, per_owner)]
    out = None
    codes = []
    for n in range(per_owner):
        acts = [across[n], across_twin[n]]
        if n == 0:
            acts = [activations, twin] + acts
        out, coded = grad_call(places[n], ids, chosen, acts, grad_out, kept, per_owner, out)
        codes.append(coded)

    lanes = freq_rows.reshape(replicas, tile_rows, tile_cols // 4, 1, 4)
    lanes = jnp.transpose(lanes, (1, 2, 3, 4, 0))
    lanes = jnp.broadcast_to(lanes, (tile_rows, tile_cols // 4, 4, 4, replicas))
    lanes = lanes.reshape(tile_rows, tile_cols // 4 * 16 * replicas)
    lanes = jnp.pad(lanes, ((0, PAD), (0, 0)))
    update = None
    for n in range(per_owner):
        near = jnp.stack([codes[n]] + [flip(codes[n], "replica", mask) for mask in range(2, replicas, 2)])
        far = flip(near, "replica", 1)
        update = update_call(places[n], ids, near, far, lanes, features, per_owner, update)

    input_grad = add_decode(own, own_twin, code, 2)
    return (input_grad, out[None], update)


def decode(coeff_all, chosen_all, basis):
    onehot = (chosen_all[..., None] == jnp.arange(TILE, dtype=jnp.int32)).astype(jnp.float32)
    summed = jnp.einsum("rack,racj->ackj", onehot, coeff_all, precision=highest)
    right_done = jnp.einsum("ackj,jm->ackm", summed, basis, precision=highest)
    decoded = jnp.einsum("kn,ackm->ancm", basis, right_done, precision=highest)
    return decoded.reshape(summed.shape[0] * TILE, summed.shape[1] * TILE)


def any_body(activations, grad_out, weight, momentum, freq_rows):
    basis = cosine_table()
    partial_value = lax.dot_general(
        grad_out, weight, (((1,), (1,)), ((), ())), preferred_element_type=jnp.float32
    )
    input_grad = lax.psum_scatter(partial_value, "tensor", scatter_dimension=1, tiled=True).astype(
        jnp.bfloat16
    )
    weight_grad = lax.dot_general(
        lax.all_gather(activations, "tensor", axis=1, tiled=True),
        grad_out,
        (((0,), (0,)), ((), ())),
        preferred_element_type=jnp.float32,
    )
    feature_count = weight_grad.shape[0]
    hidden_count = weight_grad.shape[1]
    tile_rows = feature_count // TILE
    tile_cols = hidden_count // TILE
    kept = decay_rate * momentum[0] + weight_grad
    my_index = lax.axis_index("replica")
    chosen = lax.dynamic_index_in_dim(freq_rows, my_index, 0, keepdims=False)
    tile_view = kept.reshape(tile_rows, TILE, tile_cols, TILE)
    half_done = jnp.einsum("ancm,lm->ancl", tile_view, basis, precision=highest)
    onehot = (chosen[:, :, None] == jnp.arange(TILE, dtype=jnp.int32)[None, None, :]).astype(
        jnp.float32
    )
    picked = jnp.einsum("ack,kn->acn", onehot, basis, precision=highest)
    coeff_rows = jnp.einsum("acn,ancl->acl", picked, half_done, precision=highest)
    spread = jnp.einsum("acj,jm->acm", coeff_rows, basis, precision=highest)
    removed = jnp.einsum("acn,acm->ancm", picked, spread)
    momentum_out = (kept - removed.reshape(feature_count, hidden_count))[None]
    share = tile_rows // lax.axis_size("replica")
    received = lax.all_to_all(coeff_rows[None], "replica", split_axis=1, concat_axis=0, tiled=True)
    mine_chosen = lax.dynamic_slice_in_dim(freq_rows, my_index * share, share, 1)
    band_update = decode(received, mine_chosen, basis).astype(jnp.bfloat16)
    update = lax.all_gather(band_update, "replica", axis=0, tiled=True)
    return (input_grad, momentum_out, update)


def fits(sizes, tokens, width, hidden):
    return (
        sizes["tensor"] == 4
        and sizes["replica"] == 8
        and tokens % 32 == 0
        and width == 2 * STEP
        and hidden % (4 * TILE) == 0
    )


def body(activations, grad_out, weight, momentum, freq_rows):
    sizes = {axis: lax.axis_size(axis) for axis in ("replica", "tensor")}
    fast = fits(sizes, *activations.shape, weight.shape[1])
    return (fast_body if fast else any_body)(activations, grad_out, weight, momentum, freq_rows)


def solution(mesh):
    placed = (
        P("replica", "tensor"),
        P("replica", "tensor"),
        P(None, "tensor"),
        P("replica", None, "tensor"),
        P(None, None, "tensor"),
    )
    return jax.shard_map(
        body,
        mesh=mesh,
        in_specs=placed,
        out_specs=(P("replica", "tensor"), P("replica", None, "tensor"), P(None, "tensor")),
        check_vma=False,
    )
```

```python
import functools

import jax
import jax.numpy as jnp
import numpy as np
from jax import lax
from jax.experimental import pallas as pl
from jax.experimental.pallas import tpu as pltpu
from jax.sharding import PartitionSpec as P


TILE = 64
LANES = 128
STRIP = 256
STEP = 256
PER_STEP = STEP // TILE
PAD = 8

MIB = 1 << 20


decay_rate = 0.9
highest = lax.Precision.HIGHEST


def cosine_table():
    freq = jnp.arange(TILE, dtype=jnp.float32)[:, None]
    place = jnp.arange(TILE, dtype=jnp.float32)[None, :]
    values = jnp.cos(jnp.pi * (2.0 * place + 1.0) * freq / (2.0 * TILE)) * jnp.sqrt(2.0 / TILE)
    return jnp.where(freq == 0.0, values / jnp.sqrt(2.0), values)


def cosine_constant():
    freq = np.arange(TILE)[:, None]
    place = np.arange(TILE)[None, :]
    values = np.cos(np.pi * (2 * place + 1) * freq / (2 * TILE)) * np.sqrt(2 / TILE)
    return np.where(freq == 0, values / np.sqrt(2), values).astype(np.float32)


def split3(values):
    first = values.astype(jnp.bfloat16)
    rest = values - first.astype(np.float32)
    second = rest.astype(jnp.bfloat16)
    third = (rest - second.astype(np.float32)).astype(jnp.bfloat16)
    return first, second, third


def encode(values):
    largest = jnp.maximum(jnp.max(jnp.abs(values), axis=0, keepdims=True), 1e-30)
    power = jnp.ceil(jnp.log2(largest * (1.0 / 32767.0)))
    whole = jnp.clip(jnp.round(values * jnp.exp2(-power)), -32767.0, 32767.0)
    return whole, power


def decode_block(whole, power):
    return whole * jnp.exp2(power)


def encode_rows(values):
    rows, hidden = values.shape
    lane = lax.broadcasted_iota(jnp.int32, (rows, LANES), 1)
    powers = jnp.zeros((rows, LANES), jnp.float32)
    strips = []
    for n in range(hidden // STRIP):
        strip = values[:, n * STRIP : (n + 1) * STRIP]
        largest = jnp.maximum(jnp.max(jnp.abs(strip), axis=1, keepdims=True), 1e-30)
        power = jnp.ceil(jnp.log2(largest * (1.0 / 32767.0)))
        strips.append(jnp.clip(jnp.round(strip * jnp.exp2(-power)), -32767.0, 32767.0))
        powers = jnp.where(lane == n, power, powers)
    return jnp.concatenate(strips + [powers], axis=1).astype(jnp.int32).astype(jnp.int16)


def decode_rows(code):
    code = code.astype(jnp.int32).astype(jnp.float32)
    hidden = code.shape[1] - LANES
    scale = jnp.exp2(code[:, hidden:])
    strips = [
        code[:, n * STRIP : (n + 1) * STRIP] * scale[:, n : n + 1] for n in range(hidden // STRIP)
    ]
    return jnp.concatenate(strips, axis=1)


def block_of(ids_ref, place, per_owner):
    return (ids_ref[0] ^ place[0]) * per_owner + place[1]


def grad_kernel(pieces, places, per_owner, chained, *refs):
    refs = list(refs)
    ids_ref, chosen_ref = refs[:2]
    acts_refs, refs = refs[2 : 2 + pieces], refs[2 + pieces :]
    go_ref, mom_ref, ct_ref = refs[:3]
    refs = refs[4:] if chained else refs[3:]
    out_ref, code_ref = refs[:2]
    go_buf, acts_buf, mom_buf, *g_refs, turned_ref, tab_ref, rows_ref, in_sem, out_sem = refs[2:]
    steps = len(places)
    _, hidden = go_buf.shape

    def rows_of(step):
        start = block_of(ids_ref, places[step], per_owner) * STEP
        return pl.ds(pl.multiple_of(start, STEP), STEP)

    go_copy = pltpu.make_async_copy(go_ref, go_buf, in_sem.at[2 * steps])
    go_copy.start()
    step = 0
    for piece in acts_refs:
        for n in range(piece.shape[1] // STEP):
            source = piece.at[:, pl.ds(n * STEP, STEP)]
            pltpu.make_async_copy(source, acts_buf.at[step], in_sem.at[step]).start()
            source = mom_ref.at[rows_of(step), :]
            pltpu.make_async_copy(source, mom_buf.at[step], in_sem.at[steps + step]).start()
            step += 1
    for k in range(TILE):
        tab_ref[k] = jnp.broadcast_to(ct_ref[:, k : k + 1], (TILE, LANES))
    left = lax.broadcasted_iota(jnp.int32, (TILE, LANES), 1) < TILE
    go_copy.wait()

    def wait_for(buf, sem):
        pltpu.make_async_copy(buf, buf, sem).wait()

    def turn(step):
        wait_for(acts_buf.at[step], in_sem.at[step])
        turned_ref[...] = jnp.transpose(acts_buf[step])

    def products(step, lanes):
        g_refs[step % 2][:, lanes] = jnp.dot(
            turned_ref[...], go_buf[:, lanes], preferred_element_type=jnp.float32
        )

    strips = [pl.ds(n * STRIP, STRIP) for n in range(hidden // STRIP)]
    turn(0)
    for strip in strips:
        products(0, strip)
    for step in range(steps):
        wait_for(mom_buf.at[step], in_sem.at[steps + step])
        if step + 1 < steps:
            turn(step + 1)
        block = block_of(ids_ref, places[step], per_owner)
        g_ref = g_refs[step % 2]
        for n, strip in enumerate(strips):
            if step + 1 < steps:
                products(step + 1, strip)
            for tr in range(PER_STEP):
                rows = pl.ds(tr * TILE, TILE)
                tile = block * PER_STEP + tr
                for pair in range(n * STRIP // LANES, (n + 1) * STRIP // LANES):
                    lanes = pl.ds(pair * LANES, LANES)
                    picked = jnp.where(
                        left,
                        tab_ref[chosen_ref[tile, 2 * pair]],
                        tab_ref[chosen_ref[tile, 2 * pair + 1]],
                    )
                    kept = decay_rate * mom_buf[step, rows, lanes] + g_ref[rows, lanes]
                    row = jnp.sum(kept * picked, axis=0, keepdims=True)
                    mom_buf[step, rows, lanes] = kept - picked * row
                    rows_ref[step * PER_STEP + tr, :, lanes] = row
        pltpu.make_async_copy(mom_buf.at[step], out_ref.at[rows_of(step), :], out_sem.at[step]).start()
    code_ref[...] = encode_rows(jnp.concatenate([rows_ref[n] for n in range(steps * PER_STEP)], axis=0))
    for step in range(steps):
        pltpu.make_async_copy(mom_buf.at[step], out_ref.at[rows_of(step), :], out_sem.at[step]).wait()


def grad_call(places, ids, chosen, acts, grad_out, momentum, per_owner, chained):
    tokens, hidden = grad_out.shape
    features = momentum.shape[0]
    steps = len(places)
    rows = steps * PER_STEP
    anywhere = pl.BlockSpec(memory_space=pl.ANY)
    operands = [ids, chosen, *acts, grad_out, momentum, cosine_constant().T.copy()]
    far = pl.BlockSpec(memory_space=pltpu.HBM)
    in_specs = [anywhere] * (len(acts) + 1) + [far]
    in_specs.append(pl.BlockSpec((TILE, TILE), lambda i, ids, cho: (0, 0)))
    aliases = {}
    if chained is not None:
        aliases = {len(operands): 0}
        operands.append(chained)
        in_specs.append(far)
    return pl.pallas_call(
        functools.partial(grad_kernel, len(acts), places, per_owner, chained is not None),
        grid_spec=pltpu.PrefetchScalarGridSpec(
            num_scalar_prefetch=2,
            grid=(1,),
            in_specs=in_specs,
            out_specs=[far, pl.BlockSpec((rows, hidden + LANES), lambda i, ids, cho: (0, 0))],
            scratch_shapes=[
                pltpu.VMEM((tokens, hidden), grad_out.dtype),
                pltpu.VMEM((steps, tokens, STEP), grad_out.dtype),
                pltpu.VMEM((steps, STEP, hidden), jnp.float32),
                pltpu.VMEM((STEP, hidden), jnp.float32),
                pltpu.VMEM((STEP, hidden), jnp.float32),
                pltpu.VMEM((STEP, tokens), grad_out.dtype),
                pltpu.VMEM((TILE, TILE, LANES), jnp.float32),
                pltpu.VMEM((rows + PAD, 1, hidden), jnp.float32),
                pltpu.SemaphoreType.DMA((2 * steps + 1,)),
                pltpu.SemaphoreType.DMA((steps,)),
            ],
        ),
        out_shape=[
            jax.ShapeDtypeStruct((features, hidden), jnp.float32),
            jax.ShapeDtypeStruct((rows, hidden + LANES), jnp.int16),
        ],
        input_output_aliases=aliases,
        cost_estimate=pl.CostEstimate(
            flops=2 * steps * STEP * tokens * hidden,
            bytes_accessed=2 * tokens * hidden + 8 * steps * STEP * hidden,
            transcendentals=0,
        ),
        compiler_params=pltpu.CompilerParams(
            vmem_limit_bytes=50 * MIB
        ),
        name="grad_step",
    )(*operands)


def partial_kernel(masks, ids_ref, go_ref, w_ref, *refs):
    out_refs, (go_buf, w_buf, out_buf, in_sem, out_sem) = refs[: len(masks)], refs[len(masks) :]
    chunks, rows, _ = go_buf.shape
    width = w_buf.shape[1]
    copies = []
    for n, mask in enumerate(masks):
        start = pl.multiple_of((ids_ref[0] ^ mask) * width, width)
        copies.append(pltpu.make_async_copy(w_ref.at[pl.ds(start, width), :], w_buf.at[n], in_sem.at[n]))
    for n in range(chunks):
        source = go_ref.at[pl.ds(n * rows, rows), :]
        copies.append(pltpu.make_async_copy(source, go_buf.at[n], in_sem.at[len(masks) + n]))
    for n in (0, len(masks), *range(1, len(masks)), *range(len(masks) + 1, len(copies))):
        copies[n].start()
    outs = []
    for n in range(chunks):
        copies[len(masks) + n].wait()
        for m in range(len(masks)):
            if n == 0:
                copies[m].wait()
            out_buf[m, n] = lax.dot_general(
                go_buf[n], w_buf[m], (((1,), (1,)), ((), ())), preferred_element_type=jnp.float32
            )
            target = out_refs[m].at[pl.ds(n * rows, rows), :]
            outs.append(pltpu.make_async_copy(out_buf.at[m, n], target, out_sem.at[m, n]))
            outs[-1].start()
    for copy in outs:
        copy.wait()


def partial_call(masks, ids, grad_out, weight, width):
    tokens, hidden = grad_out.shape
    chunks = 2
    rows = tokens // chunks
    shape = jax.ShapeDtypeStruct((tokens, width), jnp.float32)
    anywhere = pl.BlockSpec(memory_space=pl.ANY)
    return pl.pallas_call(
        functools.partial(partial_kernel, masks),
        grid_spec=pltpu.PrefetchScalarGridSpec(
            num_scalar_prefetch=1,
            grid=(1,),
            in_specs=[anywhere, pl.BlockSpec(memory_space=pltpu.HBM)],
            out_specs=[anywhere] * len(masks),
            scratch_shapes=[
                pltpu.VMEM((chunks, rows, hidden), grad_out.dtype),
                pltpu.VMEM((len(masks), width, hidden), weight.dtype),
                pltpu.VMEM((len(masks), chunks, rows, width), jnp.float32),
                pltpu.SemaphoreType.DMA((len(masks) + chunks,)),
                pltpu.SemaphoreType.DMA((len(masks), chunks)),
            ],
        ),
        out_shape=[shape] * len(masks),
        cost_estimate=pl.CostEstimate(
            flops=2 * len(masks) * tokens * width * hidden,
            bytes_accessed=2 * tokens * hidden + len(masks) * width * (2 * hidden + 4 * tokens),
            transcendentals=0,
        ),
        compiler_params=pltpu.CompilerParams(
            vmem_limit_bytes=57 * MIB
        ),
        name="partial_products",
    )(ids, grad_out, weight)


def add_encode_kernel(a_ref, b_ref, out_ref):
    whole, power = encode(a_ref[...] + b_ref[...])
    power = jnp.broadcast_to(power, (2 * PAD, power.shape[1]))
    rows = whole.shape[0]
    out_ref[:rows, :] = whole.astype(jnp.int32).astype(jnp.int16)
    out_ref[rows:, :] = power.astype(jnp.int32).astype(jnp.int16)


def add_encode(a, b, blocks):
    tokens, width = a.shape
    rows = tokens // blocks
    spec = pl.BlockSpec((rows, width), lambda i: (i, 0))
    return pl.pallas_call(
        add_encode_kernel,
        grid=(blocks,),
        in_specs=[spec, spec],
        out_specs=pl.BlockSpec((rows + 2 * PAD, width), lambda i: (i, 0)),
        out_shape=jax.ShapeDtypeStruct((blocks * (rows + 2 * PAD), width), jnp.int16),
        cost_estimate=pl.CostEstimate(flops=8 * a.size, bytes_accessed=10 * a.size, transcendentals=0),
        compiler_params=pltpu.CompilerParams(vmem_limit_bytes=2 * MIB + 24 * rows * width),
        name="add_encode",
    )(a, b)


def add_decode_kernel(a_ref, b_ref, code_ref, out_ref):
    rows = a_ref.shape[0]
    whole = code_ref[:rows, :].astype(jnp.int32).astype(jnp.float32)
    power = code_ref[rows:, :].astype(jnp.int32).astype(jnp.float32)[:1]
    out_ref[...] = (a_ref[...] + b_ref[...] + decode_block(whole, power)).astype(out_ref.dtype)


def add_decode(a, b, code, blocks):
    tokens, width = a.shape
    rows = tokens // blocks
    spec = pl.BlockSpec((rows, width), lambda i: (i, 0))
    return pl.pallas_call(
        add_decode_kernel,
        grid=(blocks,),
        in_specs=[spec, spec, pl.BlockSpec((rows + 2 * PAD, width), lambda i: (i, 0))],
        out_specs=spec,
        out_shape=jax.ShapeDtypeStruct((tokens, width), jnp.bfloat16),
        cost_estimate=pl.CostEstimate(flops=8 * a.size, bytes_accessed=12 * a.size, transcendentals=0),
        compiler_params=pltpu.CompilerParams(vmem_limit_bytes=2 * MIB + 28 * rows * width),
        name="add_decode",
    )(a, b, code)


def update_kernel(places, per_owner, chained, ids_ref, near_ref, far_ref, freq_ref, ct_ref, *refs):
    if chained:
        refs = refs[1:]
    out_ref, held_ref, out_buf, out_sem = refs
    steps = len(places)
    rows = steps * PER_STEP
    hidden = out_ref.shape[1]
    total = near_ref.shape[0]
    replicas = 2 * total
    for side, ref in enumerate((near_ref, far_ref)):
        for slot in range(total):
            values = decode_rows(ref[slot])
            start = pl.multiple_of((ids_ref[1] ^ (2 * slot + side)) * rows, 8)
            for strip in range(hidden // LANES):
                held_ref[strip, pl.ds(start, rows), :] = values[:, strip * LANES : (strip + 1) * LANES]

    groups = hidden // (4 * TILE)
    wide = groups * LANES
    number = lax.broadcasted_iota(jnp.int32, (TILE, wide), 0)
    main = (lax.broadcasted_iota(jnp.int32, (TILE, wide), 1) % LANES) < TILE
    lane_tile = lax.broadcasted_iota(jnp.int32, (replicas, 4 * TILE), 1) // TILE

    for step in range(steps):
        block = block_of(ids_ref, places[step], per_owner)

        def tile_row(tr, carry):
            onehot = number == freq_ref[pl.ds(block * PER_STEP + tr, 1), :]
            onehot = onehot.astype(jnp.float32).astype(jnp.bfloat16)
            columns = jnp.dot(
                ct_ref[...],
                jnp.concatenate([onehot] * 3, axis=0),
                preferred_element_type=jnp.float32,
            )
            high = columns.astype(jnp.bfloat16).astype(jnp.float32)
            lhs = jnp.where(main, high, columns - high).astype(jnp.bfloat16)
            here = step * PER_STEP + tr
            row0 = pl.ds(pl.multiple_of(tr * TILE, TILE), TILE)
            for group in range(groups):
                values = jnp.concatenate(
                    [held_ref[2 * group + n, pl.ds(here, replicas, stride=rows), :] for n in range(2)],
                    axis=1,
                )
                top = values.astype(jnp.bfloat16).astype(jnp.float32)
                low = values - top
                parts = [jnp.where(lane_tile == c, part, 0.0) for part in (top, low) for c in range(4)]
                rhs = jnp.concatenate(parts, axis=0).astype(jnp.bfloat16)
                rhs = jnp.concatenate([rhs, rhs], axis=0)
                product = jnp.dot(
                    lhs[:, group * LANES : (group + 1) * LANES], rhs, preferred_element_type=jnp.float32
                )
                lanes = pl.ds(group * 4 * TILE, 4 * TILE)
                out_buf[step, row0, lanes] = product.astype(out_buf.dtype)
            return carry

        lax.fori_loop(0, PER_STEP, tile_row, 0, unroll=True)
        target = out_ref.at[pl.ds(pl.multiple_of(block * STEP, STEP), STEP), :]
        pltpu.make_async_copy(out_buf.at[step], target, out_sem.at[step]).start()
    for step in range(steps):
        block = block_of(ids_ref, places[step], per_owner)
        target = out_ref.at[pl.ds(pl.multiple_of(block * STEP, STEP), STEP), :]
        pltpu.make_async_copy(out_buf.at[step], target, out_sem.at[step]).wait()


def update_call(places, ids, near, far, freq_lanes, features, per_owner, chained):
    hidden = near.shape[2] - LANES
    steps = len(places)
    rows = steps * PER_STEP
    anywhere = pl.BlockSpec(memory_space=pltpu.HBM)
    table = jnp.concatenate(split3(cosine_constant().T), axis=1)
    operands = [ids, near, far, freq_lanes, table]
    in_specs = [
        pl.BlockSpec(near.shape, lambda i, ids: (0, 0, 0)),
        pl.BlockSpec(far.shape, lambda i, ids: (0, 0, 0)),
        pl.BlockSpec(freq_lanes.shape, lambda i, ids: (0, 0)),
        pl.BlockSpec(table.shape, lambda i, ids: (0, 0)),
    ]
    aliases = {}
    if chained is not None:
        aliases = {len(operands): 0}
        operands.append(chained)
        in_specs.append(anywhere)
    replicas = 2 * near.shape[0]
    return pl.pallas_call(
        functools.partial(update_kernel, places, per_owner, chained is not None),
        grid_spec=pltpu.PrefetchScalarGridSpec(
            num_scalar_prefetch=1,
            grid=(1,),
            in_specs=in_specs,
            out_specs=anywhere,
            scratch_shapes=[
                pltpu.VMEM((hidden // LANES, (replicas + 1) * rows, LANES), jnp.float32),
                pltpu.VMEM((steps, STEP, hidden), jnp.bfloat16),
                pltpu.SemaphoreType.DMA((steps,)),
            ],
        ),
        out_shape=jax.ShapeDtypeStruct((features, hidden), jnp.bfloat16),
        input_output_aliases=aliases,
        cost_estimate=pl.CostEstimate(
            flops=2 * rows * TILE * 512 * hidden, bytes_accessed=2 * rows * TILE * hidden, transcendentals=0
        ),
        compiler_params=pltpu.CompilerParams(
            vmem_limit_bytes=4 * MIB + 2 * rows * TILE * hidden + 4 * (replicas + 1) * rows * hidden + 4 * near.size * 4
        ),
        name="update_rows",
    )(*operands)


def flip(x, axis, mask):
    size = lax.axis_size(axis)
    return lax.ppermute(x, axis, [(i, i ^ mask) for i in range(size)])


def fast_body(activations, grad_out, weight, momentum, freq_rows):
    return fast_layer(activations, grad_out, weight, momentum, freq_rows)


def fast_layer(activations, grad_out, weight, momentum, freq_rows):
    device = lax.axis_index("tensor")
    replica = lax.axis_index("replica")
    ids = jnp.stack([device, replica])
    features, _ = weight.shape
    width = activations.shape[1]
    per_owner = width // STEP
    tile_rows, tile_cols = freq_rows.shape[1:]
    replicas = freq_rows.shape[0]

    twin = flip(activations, "tensor", 1)
    across = flip(activations, "tensor", 2)
    across_twin = flip(across, "tensor", 1)
    sources = ((activations, twin), (across, across_twin))

    for_twin, for_far = partial_call((3, 2), ids, grad_out, weight, width)
    received = flip(for_twin, "tensor", 1)
    lanes = freq_rows.reshape(replicas, tile_rows, tile_cols // 4, 1, 4)
    lanes = jnp.transpose(lanes, (1, 2, 3, 4, 0))
    lanes = jnp.broadcast_to(lanes, (tile_rows, tile_cols // 4, 4, 4, replicas))
    lanes = lanes.reshape(tile_rows, tile_cols // 4 * 16 * replicas)
    lanes = jnp.pad(lanes, ((0, PAD), (0, 0)))
    chosen = lax.dynamic_index_in_dim(freq_rows, replica, 0, keepdims=False)
    received, lanes = lax.optimization_barrier((received, lanes))
    code = add_encode(for_far, received, 2)
    code = flip(code, "tensor", 2)
    for_twin, own = partial_call((1, 0), ids, grad_out, weight, width)
    own_twin = flip(for_twin, "tensor", 1)

    kept = momentum[0]
    places = [
        tuple((mask, n) for mask in masks for n in range(per_owner)) for masks in ((0, 1), (2, 3))
    ]
    out = None
    codes = []
    for half, acts in enumerate(sources):
        out, coded = grad_call(places[half], ids, chosen, acts, grad_out, kept, per_owner, out)
        codes.append(coded)

    update = None
    for half in range(2):
        near = jnp.stack([codes[half]] + [flip(codes[half], "replica", mask) for mask in range(2, replicas, 2)])
        far = flip(near, "replica", 1)
        update = update_call(places[half], ids, near, far, lanes, features, per_owner, update)

    input_grad = add_decode(own, own_twin, code, 2)
    return (input_grad, out[None], update)


def decode(coeff_all, chosen_all, basis):
    onehot = (chosen_all[..., None] == jnp.arange(TILE, dtype=jnp.int32)).astype(jnp.float32)
    summed = jnp.einsum("rack,racj->ackj", onehot, coeff_all, precision=highest)
    right_done = jnp.einsum("ackj,jm->ackm", summed, basis, precision=highest)
    decoded = jnp.einsum("kn,ackm->ancm", basis, right_done, precision=highest)
    return decoded.reshape(summed.shape[0] * TILE, summed.shape[1] * TILE)


def any_body(activations, grad_out, weight, momentum, freq_rows):
    basis = cosine_table()
    partial_value = lax.dot_general(
        grad_out, weight, (((1,), (1,)), ((), ())), preferred_element_type=jnp.float32
    )
    input_grad = lax.psum_scatter(partial_value, "tensor", scatter_dimension=1, tiled=True).astype(
        jnp.bfloat16
    )
    weight_grad = lax.dot_general(
        lax.all_gather(activations, "tensor", axis=1, tiled=True),
        grad_out,
        (((0,), (0,)), ((), ())),
        preferred_element_type=jnp.float32,
    )
    feature_count = weight_grad.shape[0]
    hidden_count = weight_grad.shape[1]
    tile_rows = feature_count // TILE
    tile_cols = hidden_count // TILE
    kept = decay_rate * momentum[0] + weight_grad
    my_index = lax.axis_index("replica")
    chosen = lax.dynamic_index_in_dim(freq_rows, my_index, 0, keepdims=False)
    tile_view = kept.reshape(tile_rows, TILE, tile_cols, TILE)
    half_done = jnp.einsum("ancm,lm->ancl", tile_view, basis, precision=highest)
    onehot = (chosen[:, :, None] == jnp.arange(TILE, dtype=jnp.int32)[None, None, :]).astype(
        jnp.float32
    )
    picked = jnp.einsum("ack,kn->acn", onehot, basis, precision=highest)
    coeff_rows = jnp.einsum("acn,ancl->acl", picked, half_done, precision=highest)
    spread = jnp.einsum("acj,jm->acm", coeff_rows, basis, precision=highest)
    removed = jnp.einsum("acn,acm->ancm", picked, spread)
    momentum_out = (kept - removed.reshape(feature_count, hidden_count))[None]
    share = tile_rows // lax.axis_size("replica")
    received = lax.all_to_all(coeff_rows[None], "replica", split_axis=1, concat_axis=0, tiled=True)
    mine_chosen = lax.dynamic_slice_in_dim(freq_rows, my_index * share, share, 1)
    band_update = decode(received, mine_chosen, basis).astype(jnp.bfloat16)
    update = lax.all_gather(band_update, "replica", axis=0, tiled=True)
    return (input_grad, momentum_out, update)


def fits(sizes, tokens, width, hidden):
    return (
        sizes["tensor"] == 4
        and sizes["replica"] == 8
        and tokens % 32 == 0
        and width == 2 * STEP
        and hidden % STRIP == 0
        and hidden <= STRIP * LANES
    )


def body(activations, grad_out, weight, momentum, freq_rows):
    sizes = {axis: lax.axis_size(axis) for axis in ("replica", "tensor")}
    fast = fits(sizes, *activations.shape, weight.shape[1])
    return (fast_body if fast else any_body)(activations, grad_out, weight, momentum, freq_rows)


def solution(mesh):
    placed = (
        P("replica", "tensor"),
        P("replica", "tensor"),
        P(None, "tensor"),
        P("replica", None, "tensor"),
        P(None, None, "tensor"),
    )
    return jax.shard_map(
        body,
        mesh=mesh,
        in_specs=placed,
        out_specs=(P("replica", "tensor"), P("replica", None, "tensor"), P(None, "tensor")),
        check_vma=False,
    )
```

```python
import functools

import jax
import jax.numpy as jnp
import numpy as np
from jax import lax
from jax.experimental import pallas as pl
from jax.experimental.pallas import tpu as pltpu
from jax.sharding import PartitionSpec as P


TILE = 64
LANES = 128
STRIP = 256
STEP = 256
PER_STEP = STEP // TILE
PAD = 8

MIB = 1 << 20


decay_rate = 0.9
highest = lax.Precision.HIGHEST


def cosine_table():
    freq = jnp.arange(TILE, dtype=jnp.float32)[:, None]
    place = jnp.arange(TILE, dtype=jnp.float32)[None, :]
    values = jnp.cos(jnp.pi * (2.0 * place + 1.0) * freq / (2.0 * TILE)) * jnp.sqrt(2.0 / TILE)
    return jnp.where(freq == 0.0, values / jnp.sqrt(2.0), values)


def cosine_constant():
    freq = np.arange(TILE)[:, None]
    place = np.arange(TILE)[None, :]
    values = np.cos(np.pi * (2 * place + 1) * freq / (2 * TILE)) * np.sqrt(2 / TILE)
    return np.where(freq == 0, values / np.sqrt(2), values).astype(np.float32)


def split3(values):
    first = values.astype(jnp.bfloat16)
    rest = values - first.astype(np.float32)
    second = rest.astype(jnp.bfloat16)
    third = (rest - second.astype(np.float32)).astype(jnp.bfloat16)
    return first, second, third


def encode(values):
    largest = jnp.maximum(jnp.max(jnp.abs(values), axis=0, keepdims=True), 1e-30)
    power = jnp.ceil(jnp.log2(largest * (1.0 / 32767.0)))
    whole = jnp.clip(jnp.round(values * jnp.exp2(-power)), -32767.0, 32767.0)
    return whole, power


def decode_block(whole, power):
    return whole * jnp.exp2(power)


def encode_rows(values):
    rows, hidden = values.shape
    lane = lax.broadcasted_iota(jnp.int32, (rows, LANES), 1)
    powers = jnp.zeros((rows, LANES), jnp.float32)
    strips = []
    for n in range(hidden // STRIP):
        strip = values[:, n * STRIP : (n + 1) * STRIP]
        largest = jnp.maximum(jnp.max(jnp.abs(strip), axis=1, keepdims=True), 1e-30)
        power = jnp.ceil(jnp.log2(largest * (1.0 / 32767.0)))
        strips.append(jnp.clip(jnp.round(strip * jnp.exp2(-power)), -32767.0, 32767.0))
        powers = jnp.where(lane == n, power, powers)
    return jnp.concatenate(strips + [powers], axis=1).astype(jnp.int32).astype(jnp.int16)


def decode_rows(code):
    code = code.astype(jnp.int32).astype(jnp.float32)
    hidden = code.shape[1] - LANES
    scale = jnp.exp2(code[:, hidden:])
    strips = [
        code[:, n * STRIP : (n + 1) * STRIP] * scale[:, n : n + 1] for n in range(hidden // STRIP)
    ]
    return jnp.concatenate(strips, axis=1)


def block_of(ids_ref, place, per_owner):
    return (ids_ref[0] ^ place[0]) * per_owner + place[1]


def grad_kernel(pieces, places, per_owner, chained, *refs):
    refs = list(refs)
    ids_ref, chosen_ref = refs[:2]
    acts_refs, refs = refs[2 : 2 + pieces], refs[2 + pieces :]
    go_ref, mom_ref, ct_ref = refs[:3]
    refs = refs[4:] if chained else refs[3:]
    out_ref, code_ref = refs[:2]
    go_buf, acts_buf, mom_buf, *g_refs, turned_ref, tab_ref, rows_ref, in_sem, out_sem = refs[2:]
    steps = len(places)
    _, hidden = go_buf.shape

    def rows_of(step):
        start = block_of(ids_ref, places[step], per_owner) * STEP
        return pl.ds(pl.multiple_of(start, STEP), STEP)

    go_copy = pltpu.make_async_copy(go_ref, go_buf, in_sem.at[2 * steps])
    go_copy.start()
    step = 0
    for piece in acts_refs:
        for n in range(piece.shape[1] // STEP):
            source = piece.at[:, pl.ds(n * STEP, STEP)]
            pltpu.make_async_copy(source, acts_buf.at[step], in_sem.at[step]).start()
            source = mom_ref.at[rows_of(step), :]
            pltpu.make_async_copy(source, mom_buf.at[step], in_sem.at[steps + step]).start()
            step += 1
    for k in range(TILE):
        tab_ref[k] = jnp.broadcast_to(ct_ref[:, k : k + 1], (TILE, LANES))
    left = lax.broadcasted_iota(jnp.int32, (TILE, LANES), 1) < TILE
    go_copy.wait()

    def wait_for(buf, sem):
        pltpu.make_async_copy(buf, buf, sem).wait()

    def turn(step):
        wait_for(acts_buf.at[step], in_sem.at[step])
        turned_ref[...] = jnp.transpose(acts_buf[step])

    def products(step, lanes):
        g_refs[step % 2][:, lanes] = jnp.dot(
            turned_ref[...], go_buf[:, lanes], preferred_element_type=jnp.float32
        )

    strips = [pl.ds(n * STRIP, STRIP) for n in range(hidden // STRIP)]
    turn(0)
    for strip in strips:
        products(0, strip)
    for step in range(steps):
        wait_for(mom_buf.at[step], in_sem.at[steps + step])
        if step + 1 < steps:
            turn(step + 1)
        block = block_of(ids_ref, places[step], per_owner)
        g_ref = g_refs[step % 2]
        for n, strip in enumerate(strips):
            if step + 1 < steps:
                products(step + 1, strip)
            for tr in range(PER_STEP):
                rows = pl.ds(tr * TILE, TILE)
                tile = block * PER_STEP + tr
                for pair in range(n * STRIP // LANES, (n + 1) * STRIP // LANES):
                    lanes = pl.ds(pair * LANES, LANES)
                    picked = jnp.where(
                        left,
                        tab_ref[chosen_ref[tile, 2 * pair]],
                        tab_ref[chosen_ref[tile, 2 * pair + 1]],
                    )
                    kept = decay_rate * mom_buf[step, rows, lanes] + g_ref[rows, lanes]
                    row = jnp.sum(kept * picked, axis=0, keepdims=True)
                    mom_buf[step, rows, lanes] = kept - picked * row
                    rows_ref[step * PER_STEP + tr, :, lanes] = row
        pltpu.make_async_copy(mom_buf.at[step], out_ref.at[rows_of(step), :], out_sem.at[step]).start()
    code_ref[...] = encode_rows(jnp.concatenate([rows_ref[n] for n in range(steps * PER_STEP)], axis=0))
    for step in range(steps):
        pltpu.make_async_copy(mom_buf.at[step], out_ref.at[rows_of(step), :], out_sem.at[step]).wait()


def grad_call(places, ids, chosen, acts, grad_out, momentum, per_owner, chained):
    tokens, hidden = grad_out.shape
    features = momentum.shape[0]
    steps = len(places)
    rows = steps * PER_STEP
    anywhere = pl.BlockSpec(memory_space=pl.ANY)
    operands = [ids, chosen, *acts, grad_out, momentum, cosine_constant().T.copy()]
    far = pl.BlockSpec(memory_space=pltpu.HBM)
    in_specs = [anywhere] * (len(acts) + 1) + [far]
    in_specs.append(pl.BlockSpec((TILE, TILE), lambda i, ids, cho: (0, 0)))
    aliases = {}
    if chained is not None:
        aliases = {len(operands): 0}
        operands.append(chained)
        in_specs.append(far)
    return pl.pallas_call(
        functools.partial(grad_kernel, len(acts), places, per_owner, chained is not None),
        grid_spec=pltpu.PrefetchScalarGridSpec(
            num_scalar_prefetch=2,
            grid=(1,),
            in_specs=in_specs,
            out_specs=[far, pl.BlockSpec((rows, hidden + LANES), lambda i, ids, cho: (0, 0))],
            scratch_shapes=[
                pltpu.VMEM((tokens, hidden), grad_out.dtype),
                pltpu.VMEM((steps, tokens, STEP), grad_out.dtype),
                pltpu.VMEM((steps, STEP, hidden), jnp.float32),
                pltpu.VMEM((STEP, hidden), jnp.float32),
                pltpu.VMEM((STEP, hidden), jnp.float32),
                pltpu.VMEM((STEP, tokens), grad_out.dtype),
                pltpu.VMEM((TILE, TILE, LANES), jnp.float32),
                pltpu.VMEM((rows + PAD, 1, hidden), jnp.float32),
                pltpu.SemaphoreType.DMA((2 * steps + 1,)),
                pltpu.SemaphoreType.DMA((steps,)),
            ],
        ),
        out_shape=[
            jax.ShapeDtypeStruct((features, hidden), jnp.float32),
            jax.ShapeDtypeStruct((rows, hidden + LANES), jnp.int16),
        ],
        input_output_aliases=aliases,
        cost_estimate=pl.CostEstimate(
            flops=2 * steps * STEP * tokens * hidden,
            bytes_accessed=2 * tokens * hidden + 8 * steps * STEP * hidden,
            transcendentals=0,
        ),
        compiler_params=pltpu.CompilerParams(
            vmem_limit_bytes=50 * MIB
        ),
        name="grad_step",
    )(*operands)


def partial_kernel(masks, ids_ref, go_ref, w_ref, *refs):
    out_refs, (go_buf, w_buf, out_buf, in_sem, out_sem) = refs[: len(masks)], refs[len(masks) :]
    chunks, rows, _ = go_buf.shape
    width = w_buf.shape[1]
    copies = []
    for n, mask in enumerate(masks):
        start = pl.multiple_of((ids_ref[0] ^ mask) * width, width)
        copies.append(pltpu.make_async_copy(w_ref.at[pl.ds(start, width), :], w_buf.at[n], in_sem.at[n]))
    for n in range(chunks):
        source = go_ref.at[pl.ds(n * rows, rows), :]
        copies.append(pltpu.make_async_copy(source, go_buf.at[n], in_sem.at[len(masks) + n]))
    for n in (0, len(masks), *range(1, len(masks)), *range(len(masks) + 1, len(copies))):
        copies[n].start()
    outs = []
    for n in range(chunks):
        copies[len(masks) + n].wait()
        for m in range(len(masks)):
            if n == 0:
                copies[m].wait()
            out_buf[m, n] = lax.dot_general(
                go_buf[n], w_buf[m], (((1,), (1,)), ((), ())), preferred_element_type=jnp.float32
            )
            target = out_refs[m].at[pl.ds(n * rows, rows), :]
            outs.append(pltpu.make_async_copy(out_buf.at[m, n], target, out_sem.at[m, n]))
            outs[-1].start()
    for copy in outs:
        copy.wait()


def partial_call(masks, ids, grad_out, weight, width):
    tokens, hidden = grad_out.shape
    chunks = 2
    rows = tokens // chunks
    shape = jax.ShapeDtypeStruct((tokens, width), jnp.float32)
    anywhere = pl.BlockSpec(memory_space=pl.ANY)
    return pl.pallas_call(
        functools.partial(partial_kernel, masks),
        grid_spec=pltpu.PrefetchScalarGridSpec(
            num_scalar_prefetch=1,
            grid=(1,),
            in_specs=[anywhere, pl.BlockSpec(memory_space=pltpu.HBM)],
            out_specs=[anywhere] * len(masks),
            scratch_shapes=[
                pltpu.VMEM((chunks, rows, hidden), grad_out.dtype),
                pltpu.VMEM((len(masks), width, hidden), weight.dtype),
                pltpu.VMEM((len(masks), chunks, rows, width), jnp.float32),
                pltpu.SemaphoreType.DMA((len(masks) + chunks,)),
                pltpu.SemaphoreType.DMA((len(masks), chunks)),
            ],
        ),
        out_shape=[shape] * len(masks),
        cost_estimate=pl.CostEstimate(
            flops=2 * len(masks) * tokens * width * hidden,
            bytes_accessed=2 * tokens * hidden + len(masks) * width * (2 * hidden + 4 * tokens),
            transcendentals=0,
        ),
        compiler_params=pltpu.CompilerParams(
            vmem_limit_bytes=57 * MIB
        ),
        name="partial_products",
    )(ids, grad_out, weight)


def add_encode_kernel(a_ref, b_ref, out_ref):
    whole, power = encode(a_ref[...] + b_ref[...])
    power = jnp.broadcast_to(power, (2 * PAD, power.shape[1]))
    rows = whole.shape[0]
    out_ref[:rows, :] = whole.astype(jnp.int32).astype(jnp.int16)
    out_ref[rows:, :] = power.astype(jnp.int32).astype(jnp.int16)


def add_encode(a, b, blocks):
    tokens, width = a.shape
    rows = tokens // blocks
    spec = pl.BlockSpec((rows, width), lambda i: (i, 0))
    return pl.pallas_call(
        add_encode_kernel,
        grid=(blocks,),
        in_specs=[spec, spec],
        out_specs=pl.BlockSpec((rows + 2 * PAD, width), lambda i: (i, 0)),
        out_shape=jax.ShapeDtypeStruct((blocks * (rows + 2 * PAD), width), jnp.int16),
        cost_estimate=pl.CostEstimate(flops=8 * a.size, bytes_accessed=10 * a.size, transcendentals=0),
        compiler_params=pltpu.CompilerParams(vmem_limit_bytes=2 * MIB + 24 * rows * width),
        name="add_encode",
    )(a, b)


def add_decode_kernel(a_ref, b_ref, code_ref, out_ref):
    rows = a_ref.shape[0]
    whole = code_ref[:rows, :].astype(jnp.int32).astype(jnp.float32)
    power = code_ref[rows:, :].astype(jnp.int32).astype(jnp.float32)[:1]
    out_ref[...] = (a_ref[...] + b_ref[...] + decode_block(whole, power)).astype(out_ref.dtype)


def add_decode(a, b, code, blocks):
    tokens, width = a.shape
    rows = tokens // blocks
    spec = pl.BlockSpec((rows, width), lambda i: (i, 0))
    return pl.pallas_call(
        add_decode_kernel,
        grid=(blocks,),
        in_specs=[spec, spec, pl.BlockSpec((rows + 2 * PAD, width), lambda i: (i, 0))],
        out_specs=spec,
        out_shape=jax.ShapeDtypeStruct((tokens, width), jnp.bfloat16),
        cost_estimate=pl.CostEstimate(flops=8 * a.size, bytes_accessed=12 * a.size, transcendentals=0),
        compiler_params=pltpu.CompilerParams(vmem_limit_bytes=2 * MIB + 28 * rows * width),
        name="add_decode",
    )(a, b, code)


def update_kernel(places, per_owner, chained, ids_ref, me_ref, near_ref, far_ref, freq_ref, ct_ref, *refs):
    if chained:
        refs = refs[1:]
    out_ref, held_ref, lanes_ref, out_buf, out_sem = refs
    steps = len(places)
    rows = steps * PER_STEP
    hidden = out_ref.shape[1]
    total = near_ref.shape[0]
    replicas = 2 * total
    for side, ref in enumerate((near_ref, far_ref)):
        for slot in range(total):
            values = decode_rows(ref[slot])
            start = pl.multiple_of((me_ref[0] ^ (2 * slot + side)) * rows, 8)
            for strip in range(hidden // LANES):
                held_ref[strip, pl.ds(start, rows), :] = values[:, strip * LANES : (strip + 1) * LANES]

    groups = hidden // (4 * TILE)
    wide = groups * LANES
    packed, tile_rows = freq_ref.shape
    short = 4 * replicas
    source = lax.broadcasted_iota(jnp.int32, (packed, wide), 0)
    target = lax.broadcasted_iota(jnp.int32, (packed, wide), 1)
    same = (source // short == target // LANES) & (source % short == target % short)
    lanes_ref[:tile_rows] = lax.dot_general(
        freq_ref[...].astype(jnp.float32).astype(jnp.bfloat16),
        same.astype(jnp.float32).astype(jnp.bfloat16),
        (((0,), (0,)), ((), ())),
        preferred_element_type=jnp.float32,
    )
    number = lax.broadcasted_iota(jnp.int32, (TILE, wide), 0).astype(jnp.float32)
    main = (lax.broadcasted_iota(jnp.int32, (TILE, wide), 1) % LANES) < TILE
    lane_tile = lax.broadcasted_iota(jnp.int32, (replicas, 4 * TILE), 1) // TILE

    for step in range(steps):
        block = block_of(ids_ref, places[step], per_owner)

        def tile_row(tr, carry):
            onehot = number == lanes_ref[pl.ds(block * PER_STEP + tr, 1), :]
            onehot = onehot.astype(jnp.float32).astype(jnp.bfloat16)
            columns = jnp.dot(
                ct_ref[...],
                jnp.concatenate([onehot] * 3, axis=0),
                preferred_element_type=jnp.float32,
            )
            high = columns.astype(jnp.bfloat16).astype(jnp.float32)
            lhs = jnp.where(main, high, columns - high).astype(jnp.bfloat16)
            here = step * PER_STEP + tr
            row0 = pl.ds(pl.multiple_of(tr * TILE, TILE), TILE)
            for group in range(groups):
                values = jnp.concatenate(
                    [held_ref[2 * group + n, pl.ds(here, replicas, stride=rows), :] for n in range(2)],
                    axis=1,
                )
                top = values.astype(jnp.bfloat16).astype(jnp.float32)
                low = values - top
                parts = [jnp.where(lane_tile == c, part, 0.0) for part in (top, low) for c in range(4)]
                rhs = jnp.concatenate(parts, axis=0).astype(jnp.bfloat16)
                rhs = jnp.concatenate([rhs, rhs], axis=0)
                product = jnp.dot(
                    lhs[:, group * LANES : (group + 1) * LANES], rhs, preferred_element_type=jnp.float32
                )
                lanes = pl.ds(group * 4 * TILE, 4 * TILE)
                out_buf[step, row0, lanes] = product.astype(out_buf.dtype)
            return carry

        lax.fori_loop(0, PER_STEP, tile_row, 0, unroll=True)
        target = out_ref.at[pl.ds(pl.multiple_of(block * STEP, STEP), STEP), :]
        pltpu.make_async_copy(out_buf.at[step], target, out_sem.at[step]).start()
    for step in range(steps):
        block = block_of(ids_ref, places[step], per_owner)
        target = out_ref.at[pl.ds(pl.multiple_of(block * STEP, STEP), STEP), :]
        pltpu.make_async_copy(out_buf.at[step], target, out_sem.at[step]).wait()


def update_call(places, ids, me, near, far, freq_lanes, features, per_owner, chained):
    hidden = near.shape[2] - LANES
    steps = len(places)
    rows = steps * PER_STEP
    anywhere = pl.BlockSpec(memory_space=pltpu.HBM)
    table = jnp.concatenate(split3(cosine_constant().T), axis=1)
    operands = [ids, me, near, far, freq_lanes, table]
    in_specs = [
        pl.BlockSpec(near.shape, lambda i, ids, me: (0, 0, 0)),
        pl.BlockSpec(far.shape, lambda i, ids, me: (0, 0, 0)),
        pl.BlockSpec(freq_lanes.shape, lambda i, ids, me: (0, 0)),
        pl.BlockSpec(table.shape, lambda i, ids, me: (0, 0)),
    ]
    aliases = {}
    if chained is not None:
        aliases = {len(operands): 0}
        operands.append(chained)
        in_specs.append(anywhere)
    replicas = 2 * near.shape[0]
    return pl.pallas_call(
        functools.partial(update_kernel, places, per_owner, chained is not None),
        grid_spec=pltpu.PrefetchScalarGridSpec(
            num_scalar_prefetch=2,
            grid=(1,),
            in_specs=in_specs,
            out_specs=anywhere,
            scratch_shapes=[
                pltpu.VMEM((hidden // LANES, (replicas + 1) * rows, LANES), jnp.float32),
                pltpu.VMEM((freq_lanes.shape[1] + PAD, hidden // STRIP * LANES), jnp.float32),
                pltpu.VMEM((steps, STEP, hidden), jnp.bfloat16),
                pltpu.SemaphoreType.DMA((steps,)),
            ],
        ),
        out_shape=jax.ShapeDtypeStruct((features, hidden), jnp.bfloat16),
        input_output_aliases=aliases,
        cost_estimate=pl.CostEstimate(
            flops=2 * rows * TILE * 512 * hidden, bytes_accessed=2 * rows * TILE * hidden, transcendentals=0
        ),
        compiler_params=pltpu.CompilerParams(
            vmem_limit_bytes=4 * MIB + 2 * rows * TILE * hidden + 4 * (replicas + 1) * rows * hidden + 4 * near.size * 4
        ),
        name="update_rows",
    )(*operands)


def flip(x, axis, mask):
    size = lax.axis_size(axis)
    return lax.ppermute(x, axis, [(i, i ^ mask) for i in range(size)])


def fast_body(activations, grad_out, weight, momentum, freq_rows):
    return fast_layer(activations, grad_out, weight, momentum, freq_rows)


def fast_layer(activations, grad_out, weight, momentum, freq_rows):
    device = lax.axis_index("tensor")
    replica = lax.axis_index("replica")
    ids, me = device[None], replica[None]
    features, _ = weight.shape
    width = activations.shape[1]
    per_owner = width // STEP
    tile_rows, tile_cols = freq_rows.shape[1:]
    replicas = freq_rows.shape[0]

    twin = flip(activations, "tensor", 1)
    across = flip(activations, "tensor", 2)
    across_twin = flip(across, "tensor", 1)
    sources = ((activations, twin), (across, across_twin))

    for_twin, for_far = partial_call((3, 2), ids, grad_out, weight, width)
    received = flip(for_twin, "tensor", 1)
    chosen = lax.dynamic_index_in_dim(freq_rows, replica, 0, keepdims=False)
    lanes = jnp.transpose(freq_rows, (2, 0, 1)).reshape(tile_cols * replicas, tile_rows)
    code = add_encode(for_far, received, 2)
    code = flip(code, "tensor", 2)
    for_twin, own = partial_call((1, 0), ids, grad_out, weight, width)
    own_twin = flip(for_twin, "tensor", 1)

    kept = momentum[0]
    places = [
        tuple((mask, n) for mask in masks for n in range(per_owner)) for masks in ((0, 1), (2, 3))
    ]
    out = None
    codes = []
    for half, acts in enumerate(sources):
        out, coded = grad_call(places[half], ids, chosen, acts, grad_out, kept, per_owner, out)
        codes.append(coded)

    update = None
    for half in range(2):
        near = jnp.stack([codes[half]] + [flip(codes[half], "replica", mask) for mask in range(2, replicas, 2)])
        far = flip(near, "replica", 1)
        update = update_call(places[half], ids, me, near, far, lanes, features, per_owner, update)

    input_grad = add_decode(own, own_twin, code, 2)
    return (input_grad, out[None], update)


def decode(coeff_all, chosen_all, basis):
    onehot = (chosen_all[..., None] == jnp.arange(TILE, dtype=jnp.int32)).astype(jnp.float32)
    summed = jnp.einsum("rack,racj->ackj", onehot, coeff_all, precision=highest)
    right_done = jnp.einsum("ackj,jm->ackm", summed, basis, precision=highest)
    decoded = jnp.einsum("kn,ackm->ancm", basis, right_done, precision=highest)
    return decoded.reshape(summed.shape[0] * TILE, summed.shape[1] * TILE)


def any_body(activations, grad_out, weight, momentum, freq_rows):
    basis = cosine_table()
    partial_value = lax.dot_general(
        grad_out, weight, (((1,), (1,)), ((), ())), preferred_element_type=jnp.float32
    )
    input_grad = lax.psum_scatter(partial_value, "tensor", scatter_dimension=1, tiled=True).astype(
        jnp.bfloat16
    )
    weight_grad = lax.dot_general(
        lax.all_gather(activations, "tensor", axis=1, tiled=True),
        grad_out,
        (((0,), (0,)), ((), ())),
        preferred_element_type=jnp.float32,
    )
    feature_count = weight_grad.shape[0]
    hidden_count = weight_grad.shape[1]
    tile_rows = feature_count // TILE
    tile_cols = hidden_count // TILE
    kept = decay_rate * momentum[0] + weight_grad
    my_index = lax.axis_index("replica")
    chosen = lax.dynamic_index_in_dim(freq_rows, my_index, 0, keepdims=False)
    tile_view = kept.reshape(tile_rows, TILE, tile_cols, TILE)
    half_done = jnp.einsum("ancm,lm->ancl", tile_view, basis, precision=highest)
    onehot = (chosen[:, :, None] == jnp.arange(TILE, dtype=jnp.int32)[None, None, :]).astype(
        jnp.float32
    )
    picked = jnp.einsum("ack,kn->acn", onehot, basis, precision=highest)
    coeff_rows = jnp.einsum("acn,ancl->acl", picked, half_done, precision=highest)
    spread = jnp.einsum("acj,jm->acm", coeff_rows, basis, precision=highest)
    removed = jnp.einsum("acn,acm->ancm", picked, spread)
    momentum_out = (kept - removed.reshape(feature_count, hidden_count))[None]
    share = tile_rows // lax.axis_size("replica")
    received = lax.all_to_all(coeff_rows[None], "replica", split_axis=1, concat_axis=0, tiled=True)
    mine_chosen = lax.dynamic_slice_in_dim(freq_rows, my_index * share, share, 1)
    band_update = decode(received, mine_chosen, basis).astype(jnp.bfloat16)
    update = lax.all_gather(band_update, "replica", axis=0, tiled=True)
    return (input_grad, momentum_out, update)


def fits(sizes, tokens, width, hidden):
    return (
        sizes["tensor"] == 4
        and sizes["replica"] == 8
        and tokens % 32 == 0
        and width == 2 * STEP
        and hidden % STRIP == 0
        and hidden <= STRIP * LANES
    )


def body(activations, grad_out, weight, momentum, freq_rows):
    sizes = {axis: lax.axis_size(axis) for axis in ("replica", "tensor")}
    fast = fits(sizes, *activations.shape, weight.shape[1])
    return (fast_body if fast else any_body)(activations, grad_out, weight, momentum, freq_rows)


def solution(mesh):
    placed = (
        P("replica", "tensor"),
        P("replica", "tensor"),
        P(None, "tensor"),
        P("replica", None, "tensor"),
        P(None, None, "tensor"),
    )
    return jax.shard_map(
        body,
        mesh=mesh,
        in_specs=placed,
        out_specs=(P("replica", "tensor"), P("replica", None, "tensor"), P(None, "tensor")),
        check_vma=False,
    )
```

```python
import functools

import jax
import jax.numpy as jnp
import numpy as np
from jax import lax
from jax.experimental import pallas as pl
from jax.experimental.pallas import tpu as pltpu
from jax.sharding import PartitionSpec as P


TILE = 64
LANES = 128
STRIP = 256
STEP = 256
PER_STEP = STEP // TILE
PAD = 8

MIB = 1 << 20


decay_rate = 0.9
highest = lax.Precision.HIGHEST


def cosine_table():
    freq = jnp.arange(TILE, dtype=jnp.float32)[:, None]
    place = jnp.arange(TILE, dtype=jnp.float32)[None, :]
    values = jnp.cos(jnp.pi * (2.0 * place + 1.0) * freq / (2.0 * TILE)) * jnp.sqrt(2.0 / TILE)
    return jnp.where(freq == 0.0, values / jnp.sqrt(2.0), values)


def cosine_constant():
    freq = np.arange(TILE)[:, None]
    place = np.arange(TILE)[None, :]
    values = np.cos(np.pi * (2 * place + 1) * freq / (2 * TILE)) * np.sqrt(2 / TILE)
    return np.where(freq == 0, values / np.sqrt(2), values).astype(np.float32)


def split3(values):
    first = values.astype(jnp.bfloat16)
    rest = values - first.astype(np.float32)
    second = rest.astype(jnp.bfloat16)
    third = (rest - second.astype(np.float32)).astype(jnp.bfloat16)
    return first, second, third


def encode(values):
    largest = jnp.maximum(jnp.max(jnp.abs(values), axis=0, keepdims=True), 1e-30)
    power = jnp.ceil(jnp.log2(largest * (1.0 / 32767.0)))
    whole = jnp.clip(jnp.round(values * jnp.exp2(-power)), -32767.0, 32767.0)
    return whole, power


def decode_block(whole, power):
    return whole * jnp.exp2(power)


def encode_rows(values):
    rows, hidden = values.shape
    lane = lax.broadcasted_iota(jnp.int32, (rows, LANES), 1)
    powers = jnp.zeros((rows, LANES), jnp.float32)
    strips = []
    for n in range(hidden // STRIP):
        strip = values[:, n * STRIP : (n + 1) * STRIP]
        largest = jnp.maximum(jnp.max(jnp.abs(strip), axis=1, keepdims=True), 1e-30)
        power = jnp.ceil(jnp.log2(largest * (1.0 / 32767.0)))
        strips.append(jnp.clip(jnp.round(strip * jnp.exp2(-power)), -32767.0, 32767.0))
        powers = jnp.where(lane == n, power, powers)
    return jnp.concatenate(strips + [powers], axis=1).astype(jnp.int32).astype(jnp.int16)


def decode_rows(code):
    code = code.astype(jnp.int32).astype(jnp.float32)
    hidden = code.shape[1] - LANES
    scale = jnp.exp2(code[:, hidden:])
    strips = [
        code[:, n * STRIP : (n + 1) * STRIP] * scale[:, n : n + 1] for n in range(hidden // STRIP)
    ]
    return jnp.concatenate(strips, axis=1)


def block_of(ids_ref, place, per_owner):
    return (ids_ref[0] ^ place[0]) * per_owner + place[1]


def grad_kernel(pieces, places, per_owner, chained, *refs):
    refs = list(refs)
    ids_ref, chosen_ref = refs[:2]
    acts_refs, refs = refs[2 : 2 + pieces], refs[2 + pieces :]
    go_ref, mom_ref, ct_ref = refs[:3]
    refs = refs[4:] if chained else refs[3:]
    out_ref, code_ref = refs[:2]
    go_buf, acts_buf, mom_buf, *g_refs, turned_ref, tab_ref, rows_ref, in_sem, out_sem = refs[2:]
    steps = len(places)
    _, hidden = go_buf.shape

    def rows_of(step):
        start = block_of(ids_ref, places[step], per_owner) * STEP
        return pl.ds(pl.multiple_of(start, STEP), STEP)

    go_copy = pltpu.make_async_copy(go_ref, go_buf, in_sem.at[2 * steps])
    go_copy.start()
    step = 0
    for piece in acts_refs:
        for n in range(piece.shape[1] // STEP):
            source = piece.at[:, pl.ds(n * STEP, STEP)]
            pltpu.make_async_copy(source, acts_buf.at[step], in_sem.at[step]).start()
            source = mom_ref.at[rows_of(step), :]
            pltpu.make_async_copy(source, mom_buf.at[step], in_sem.at[steps + step]).start()
            step += 1
    for k in range(TILE):
        tab_ref[k] = jnp.broadcast_to(ct_ref[:, k : k + 1], (TILE, LANES))
    left = lax.broadcasted_iota(jnp.int32, (TILE, LANES), 1) < TILE
    go_copy.wait()

    def wait_for(buf, sem):
        pltpu.make_async_copy(buf, buf, sem).wait()

    def turn(step):
        wait_for(acts_buf.at[step], in_sem.at[step])
        turned_ref[...] = jnp.transpose(acts_buf[step])

    def products(step, lanes):
        g_refs[step % 2][:, lanes] = jnp.dot(
            turned_ref[...], go_buf[:, lanes], preferred_element_type=jnp.float32
        )

    strips = [pl.ds(n * STRIP, STRIP) for n in range(hidden // STRIP)]
    turn(0)
    for strip in strips:
        products(0, strip)
    for step in range(steps):
        wait_for(mom_buf.at[step], in_sem.at[steps + step])
        if step + 1 < steps:
            turn(step + 1)
        block = block_of(ids_ref, places[step], per_owner)
        g_ref = g_refs[step % 2]
        for n, strip in enumerate(strips):
            if step + 1 < steps:
                products(step + 1, strip)
            for tr in range(PER_STEP):
                rows = pl.ds(tr * TILE, TILE)
                tile = block * PER_STEP + tr
                for pair in range(n * STRIP // LANES, (n + 1) * STRIP // LANES):
                    lanes = pl.ds(pair * LANES, LANES)
                    picked = jnp.where(
                        left,
                        tab_ref[chosen_ref[tile, 2 * pair]],
                        tab_ref[chosen_ref[tile, 2 * pair + 1]],
                    )
                    kept = decay_rate * mom_buf[step, rows, lanes] + g_ref[rows, lanes]
                    row = jnp.sum(kept * picked, axis=0, keepdims=True)
                    mom_buf[step, rows, lanes] = kept - picked * row
                    rows_ref[step * PER_STEP + tr, :, lanes] = row
        pltpu.make_async_copy(mom_buf.at[step], out_ref.at[rows_of(step), :], out_sem.at[step]).start()
    code_ref[...] = encode_rows(jnp.concatenate([rows_ref[n] for n in range(steps * PER_STEP)], axis=0))
    for step in range(steps):
        pltpu.make_async_copy(mom_buf.at[step], out_ref.at[rows_of(step), :], out_sem.at[step]).wait()


def grad_call(places, ids, chosen, acts, grad_out, momentum, per_owner, chained):
    tokens, hidden = grad_out.shape
    features = momentum.shape[0]
    steps = len(places)
    rows = steps * PER_STEP
    anywhere = pl.BlockSpec(memory_space=pl.ANY)
    operands = [ids, chosen, *acts, grad_out, momentum, cosine_constant().T.copy()]
    far = pl.BlockSpec(memory_space=pltpu.HBM)
    in_specs = [anywhere] * (len(acts) + 1) + [far]
    in_specs.append(pl.BlockSpec((TILE, TILE), lambda i, ids, cho: (0, 0)))
    aliases = {}
    if chained is not None:
        aliases = {len(operands): 0}
        operands.append(chained)
        in_specs.append(far)
    return pl.pallas_call(
        functools.partial(grad_kernel, len(acts), places, per_owner, chained is not None),
        grid_spec=pltpu.PrefetchScalarGridSpec(
            num_scalar_prefetch=2,
            grid=(1,),
            in_specs=in_specs,
            out_specs=[far, pl.BlockSpec((rows, hidden + LANES), lambda i, ids, cho: (0, 0))],
            scratch_shapes=[
                pltpu.VMEM((tokens, hidden), grad_out.dtype),
                pltpu.VMEM((steps, tokens, STEP), grad_out.dtype),
                pltpu.VMEM((steps, STEP, hidden), jnp.float32),
                pltpu.VMEM((STEP, hidden), jnp.float32),
                pltpu.VMEM((STEP, hidden), jnp.float32),
                pltpu.VMEM((STEP, tokens), grad_out.dtype),
                pltpu.VMEM((TILE, TILE, LANES), jnp.float32),
                pltpu.VMEM((rows + PAD, 1, hidden), jnp.float32),
                pltpu.SemaphoreType.DMA((2 * steps + 1,)),
                pltpu.SemaphoreType.DMA((steps,)),
            ],
        ),
        out_shape=[
            jax.ShapeDtypeStruct((features, hidden), jnp.float32),
            jax.ShapeDtypeStruct((rows, hidden + LANES), jnp.int16),
        ],
        input_output_aliases=aliases,
        cost_estimate=pl.CostEstimate(
            flops=2 * steps * STEP * tokens * hidden,
            bytes_accessed=2 * tokens * hidden + 8 * steps * STEP * hidden,
            transcendentals=0,
        ),
        compiler_params=pltpu.CompilerParams(
            vmem_limit_bytes=50 * MIB
        ),
        name="grad_step",
    )(*operands)


def partial_kernel(masks, ids_ref, go_ref, w_ref, *refs):
    out_refs, (go_buf, w_buf, out_buf, in_sem, out_sem) = refs[: len(masks)], refs[len(masks) :]
    chunks, rows, hidden = go_buf.shape
    width = w_buf.shape[1]
    copies = []
    for n, mask in enumerate(masks):
        start = pl.multiple_of((ids_ref[0] ^ mask) * width, width)
        copies.append(pltpu.make_async_copy(w_ref.at[pl.ds(start, width), :], w_buf.at[n], in_sem.at[n]))
    for n in range(chunks):
        source = go_ref.at[pl.ds(n * rows, rows), :]
        copies.append(pltpu.make_async_copy(source, go_buf.at[n], in_sem.at[len(masks) + n]))
    for n in (0, len(masks), *range(1, len(masks)), *range(len(masks) + 1, len(copies))):
        copies[n].start()
    outs = []
    for m in range(len(masks)):
        copies[m].wait()
    for n in range(chunks):
        copies[len(masks) + n].wait()
        product = lax.dot_general(
            go_buf[n],
            w_buf[...].reshape(len(masks) * width, hidden),
            (((1,), (1,)), ((), ())),
            preferred_element_type=jnp.float32,
        )
        for m in range(len(masks)):
            out_buf[m, n] = product[:, m * width : (m + 1) * width]
            target = out_refs[m].at[pl.ds(n * rows, rows), :]
            outs.append(pltpu.make_async_copy(out_buf.at[m, n], target, out_sem.at[m, n]))
            outs[-1].start()
    for copy in outs:
        copy.wait()


def partial_call(masks, ids, grad_out, weight, width):
    tokens, hidden = grad_out.shape
    chunks = 2
    rows = tokens // chunks
    shape = jax.ShapeDtypeStruct((tokens, width), jnp.float32)
    anywhere = pl.BlockSpec(memory_space=pl.ANY)
    return pl.pallas_call(
        functools.partial(partial_kernel, masks),
        grid_spec=pltpu.PrefetchScalarGridSpec(
            num_scalar_prefetch=1,
            grid=(1,),
            in_specs=[anywhere, pl.BlockSpec(memory_space=pltpu.HBM)],
            out_specs=[anywhere] * len(masks),
            scratch_shapes=[
                pltpu.VMEM((chunks, rows, hidden), grad_out.dtype),
                pltpu.VMEM((len(masks), width, hidden), weight.dtype),
                pltpu.VMEM((len(masks), chunks, rows, width), jnp.float32),
                pltpu.SemaphoreType.DMA((len(masks) + chunks,)),
                pltpu.SemaphoreType.DMA((len(masks), chunks)),
            ],
        ),
        out_shape=[shape] * len(masks),
        cost_estimate=pl.CostEstimate(
            flops=2 * len(masks) * tokens * width * hidden,
            bytes_accessed=2 * tokens * hidden + len(masks) * width * (2 * hidden + 4 * tokens),
            transcendentals=0,
        ),
        compiler_params=pltpu.CompilerParams(
            vmem_limit_bytes=57 * MIB
        ),
        name="partial_products",
    )(ids, grad_out, weight)


def add_encode_kernel(a_ref, b_ref, out_ref):
    whole, power = encode(a_ref[...] + b_ref[...])
    power = jnp.broadcast_to(power, (2 * PAD, power.shape[1]))
    rows = whole.shape[0]
    out_ref[:rows, :] = whole.astype(jnp.int32).astype(jnp.int16)
    out_ref[rows:, :] = power.astype(jnp.int32).astype(jnp.int16)


def add_encode(a, b, blocks):
    tokens, width = a.shape
    rows = tokens // blocks
    spec = pl.BlockSpec((rows, width), lambda i: (i, 0))
    return pl.pallas_call(
        add_encode_kernel,
        grid=(blocks,),
        in_specs=[spec, spec],
        out_specs=pl.BlockSpec((rows + 2 * PAD, width), lambda i: (i, 0)),
        out_shape=jax.ShapeDtypeStruct((blocks * (rows + 2 * PAD), width), jnp.int16),
        cost_estimate=pl.CostEstimate(flops=8 * a.size, bytes_accessed=10 * a.size, transcendentals=0),
        compiler_params=pltpu.CompilerParams(vmem_limit_bytes=2 * MIB + 24 * rows * width),
        name="add_encode",
    )(a, b)


def add_decode_kernel(a_ref, b_ref, code_ref, out_ref):
    rows = a_ref.shape[0]
    whole = code_ref[:rows, :].astype(jnp.int32).astype(jnp.float32)
    power = code_ref[rows:, :].astype(jnp.int32).astype(jnp.float32)[:1]
    out_ref[...] = (a_ref[...] + b_ref[...] + decode_block(whole, power)).astype(out_ref.dtype)


def add_decode(a, b, code, blocks):
    tokens, width = a.shape
    rows = tokens // blocks
    spec = pl.BlockSpec((rows, width), lambda i: (i, 0))
    return pl.pallas_call(
        add_decode_kernel,
        grid=(blocks,),
        in_specs=[spec, spec, pl.BlockSpec((rows + 2 * PAD, width), lambda i: (i, 0))],
        out_specs=spec,
        out_shape=jax.ShapeDtypeStruct((tokens, width), jnp.bfloat16),
        cost_estimate=pl.CostEstimate(flops=8 * a.size, bytes_accessed=12 * a.size, transcendentals=0),
        compiler_params=pltpu.CompilerParams(vmem_limit_bytes=2 * MIB + 28 * rows * width),
        name="add_decode",
    )(a, b, code)


def update_kernel(places, per_owner, chained, ids_ref, me_ref, near_ref, far_ref, freq_ref, ct_ref, *refs):
    if chained:
        refs = refs[1:]
    out_ref, held_ref, lanes_ref, out_buf, out_sem = refs
    steps = len(places)
    rows = steps * PER_STEP
    hidden = out_ref.shape[1]
    total = near_ref.shape[0]
    replicas = 2 * total
    for side, ref in enumerate((near_ref, far_ref)):
        for slot in range(total):
            values = decode_rows(ref[slot])
            start = pl.multiple_of((me_ref[0] ^ (2 * slot + side)) * rows, 8)
            for strip in range(hidden // LANES):
                held_ref[strip, pl.ds(start, rows), :] = values[:, strip * LANES : (strip + 1) * LANES]

    groups = hidden // (4 * TILE)
    wide = groups * LANES
    packed, tile_rows = freq_ref.shape
    short = 4 * replicas
    source = lax.broadcasted_iota(jnp.int32, (packed, wide), 0)
    target = lax.broadcasted_iota(jnp.int32, (packed, wide), 1)
    same = (source // short == target // LANES) & (source % short == target % short)
    lanes_ref[:tile_rows] = lax.dot_general(
        freq_ref[...].astype(jnp.float32).astype(jnp.bfloat16),
        same.astype(jnp.float32).astype(jnp.bfloat16),
        (((0,), (0,)), ((), ())),
        preferred_element_type=jnp.float32,
    )
    number = lax.broadcasted_iota(jnp.int32, (TILE, wide), 0).astype(jnp.float32)
    main = (lax.broadcasted_iota(jnp.int32, (TILE, wide), 1) % LANES) < TILE
    lane_tile = lax.broadcasted_iota(jnp.int32, (replicas, 4 * TILE), 1) // TILE

    for step in range(steps):
        block = block_of(ids_ref, places[step], per_owner)

        def tile_row(tr, carry):
            onehot = number == lanes_ref[pl.ds(block * PER_STEP + tr, 1), :]
            onehot = onehot.astype(jnp.float32).astype(jnp.bfloat16)
            columns = jnp.dot(
                ct_ref[...],
                jnp.concatenate([onehot] * 3, axis=0),
                preferred_element_type=jnp.float32,
            )
            high = columns.astype(jnp.bfloat16).astype(jnp.float32)
            lhs = jnp.where(main, high, columns - high).astype(jnp.bfloat16)
            here = step * PER_STEP + tr
            row0 = pl.ds(pl.multiple_of(tr * TILE, TILE), TILE)
            for group in range(groups):
                values = jnp.concatenate(
                    [held_ref[2 * group + n, pl.ds(here, replicas, stride=rows), :] for n in range(2)],
                    axis=1,
                )
                top = values.astype(jnp.bfloat16).astype(jnp.float32)
                low = values - top
                parts = [jnp.where(lane_tile == c, part, 0.0) for part in (top, low) for c in range(4)]
                rhs = jnp.concatenate(parts, axis=0).astype(jnp.bfloat16)
                rhs = jnp.concatenate([rhs, rhs], axis=0)
                product = jnp.dot(
                    lhs[:, group * LANES : (group + 1) * LANES], rhs, preferred_element_type=jnp.float32
                )
                lanes = pl.ds(group * 4 * TILE, 4 * TILE)
                out_buf[step, row0, lanes] = product.astype(out_buf.dtype)
            return carry

        lax.fori_loop(0, PER_STEP, tile_row, 0, unroll=True)
        target = out_ref.at[pl.ds(pl.multiple_of(block * STEP, STEP), STEP), :]
        pltpu.make_async_copy(out_buf.at[step], target, out_sem.at[step]).start()
    for step in range(steps):
        block = block_of(ids_ref, places[step], per_owner)
        target = out_ref.at[pl.ds(pl.multiple_of(block * STEP, STEP), STEP), :]
        pltpu.make_async_copy(out_buf.at[step], target, out_sem.at[step]).wait()


def update_call(places, ids, me, near, far, freq_lanes, features, per_owner, chained):
    hidden = near.shape[2] - LANES
    steps = len(places)
    rows = steps * PER_STEP
    anywhere = pl.BlockSpec(memory_space=pltpu.HBM)
    table = jnp.concatenate(split3(cosine_constant().T), axis=1)
    operands = [ids, me, near, far, freq_lanes, table]
    in_specs = [
        pl.BlockSpec(near.shape, lambda i, ids, me: (0, 0, 0)),
        pl.BlockSpec(far.shape, lambda i, ids, me: (0, 0, 0)),
        pl.BlockSpec(freq_lanes.shape, lambda i, ids, me: (0, 0)),
        pl.BlockSpec(table.shape, lambda i, ids, me: (0, 0)),
    ]
    aliases = {}
    if chained is not None:
        aliases = {len(operands): 0}
        operands.append(chained)
        in_specs.append(anywhere)
    replicas = 2 * near.shape[0]
    return pl.pallas_call(
        functools.partial(update_kernel, places, per_owner, chained is not None),
        grid_spec=pltpu.PrefetchScalarGridSpec(
            num_scalar_prefetch=2,
            grid=(1,),
            in_specs=in_specs,
            out_specs=anywhere,
            scratch_shapes=[
                pltpu.VMEM((hidden // LANES, (replicas + 1) * rows, LANES), jnp.float32),
                pltpu.VMEM((freq_lanes.shape[1] + PAD, hidden // STRIP * LANES), jnp.float32),
                pltpu.VMEM((steps, STEP, hidden), jnp.bfloat16),
                pltpu.SemaphoreType.DMA((steps,)),
            ],
        ),
        out_shape=jax.ShapeDtypeStruct((features, hidden), jnp.bfloat16),
        input_output_aliases=aliases,
        cost_estimate=pl.CostEstimate(
            flops=2 * rows * TILE * 512 * hidden, bytes_accessed=2 * rows * TILE * hidden, transcendentals=0
        ),
        compiler_params=pltpu.CompilerParams(
            vmem_limit_bytes=4 * MIB + 2 * rows * TILE * hidden + 4 * (replicas + 1) * rows * hidden + 4 * near.size * 4
        ),
        name="update_rows",
    )(*operands)


def flip(x, axis, mask):
    size = lax.axis_size(axis)
    return lax.ppermute(x, axis, [(i, i ^ mask) for i in range(size)])


def fast_body(activations, grad_out, weight, momentum, freq_rows):
    return fast_layer(activations, grad_out, weight, momentum, freq_rows)


def fast_layer(activations, grad_out, weight, momentum, freq_rows):
    device = lax.axis_index("tensor")
    replica = lax.axis_index("replica")
    ids, me = device[None], replica[None]
    features, _ = weight.shape
    width = activations.shape[1]
    per_owner = width // STEP
    tile_rows, tile_cols = freq_rows.shape[1:]
    replicas = freq_rows.shape[0]

    twin = flip(activations, "tensor", 1)
    across = flip(activations, "tensor", 2)
    across_twin = flip(across, "tensor", 1)
    sources = ((activations, twin), (across, across_twin))

    for_twin, for_far = partial_call((3, 2), ids, grad_out, weight, width)
    received = flip(for_twin, "tensor", 1)
    chosen = lax.dynamic_index_in_dim(freq_rows, replica, 0, keepdims=False)
    lanes = jnp.transpose(freq_rows, (2, 0, 1)).reshape(tile_cols * replicas, tile_rows)
    code = add_encode(for_far, received, 2)
    code = flip(code, "tensor", 2)
    for_twin, own = partial_call((1, 0), ids, grad_out, weight, width)
    own_twin = flip(for_twin, "tensor", 1)

    kept = momentum[0]
    places = [
        tuple((mask, n) for mask in masks for n in range(per_owner)) for masks in ((0, 1), (2, 3))
    ]
    out = None
    codes = []
    for half, acts in enumerate(sources):
        out, coded = grad_call(places[half], ids, chosen, acts, grad_out, kept, per_owner, out)
        codes.append(coded)

    update = None
    for half in range(2):
        near = jnp.stack([codes[half]] + [flip(codes[half], "replica", mask) for mask in range(2, replicas, 2)])
        far = flip(near, "replica", 1)
        update = update_call(places[half], ids, me, near, far, lanes, features, per_owner, update)

    input_grad = add_decode(own, own_twin, code, 2)
    return (input_grad, out[None], update)


def decode(coeff_all, chosen_all, basis):
    onehot = (chosen_all[..., None] == jnp.arange(TILE, dtype=jnp.int32)).astype(jnp.float32)
    summed = jnp.einsum("rack,racj->ackj", onehot, coeff_all, precision=highest)
    right_done = jnp.einsum("ackj,jm->ackm", summed, basis, precision=highest)
    decoded = jnp.einsum("kn,ackm->ancm", basis, right_done, precision=highest)
    return decoded.reshape(summed.shape[0] * TILE, summed.shape[1] * TILE)


def any_body(activations, grad_out, weight, momentum, freq_rows):
    basis = cosine_table()
    partial_value = lax.dot_general(
        grad_out, weight, (((1,), (1,)), ((), ())), preferred_element_type=jnp.float32
    )
    input_grad = lax.psum_scatter(partial_value, "tensor", scatter_dimension=1, tiled=True).astype(
        jnp.bfloat16
    )
    weight_grad = lax.dot_general(
        lax.all_gather(activations, "tensor", axis=1, tiled=True),
        grad_out,
        (((0,), (0,)), ((), ())),
        preferred_element_type=jnp.float32,
    )
    feature_count = weight_grad.shape[0]
    hidden_count = weight_grad.shape[1]
    tile_rows = feature_count // TILE
    tile_cols = hidden_count // TILE
    kept = decay_rate * momentum[0] + weight_grad
    my_index = lax.axis_index("replica")
    chosen = lax.dynamic_index_in_dim(freq_rows, my_index, 0, keepdims=False)
    tile_view = kept.reshape(tile_rows, TILE, tile_cols, TILE)
    half_done = jnp.einsum("ancm,lm->ancl", tile_view, basis, precision=highest)
    onehot = (chosen[:, :, None] == jnp.arange(TILE, dtype=jnp.int32)[None, None, :]).astype(
        jnp.float32
    )
    picked = jnp.einsum("ack,kn->acn", onehot, basis, precision=highest)
    coeff_rows = jnp.einsum("acn,ancl->acl", picked, half_done, precision=highest)
    spread = jnp.einsum("acj,jm->acm", coeff_rows, basis, precision=highest)
    removed = jnp.einsum("acn,acm->ancm", picked, spread)
    momentum_out = (kept - removed.reshape(feature_count, hidden_count))[None]
    share = tile_rows // lax.axis_size("replica")
    received = lax.all_to_all(coeff_rows[None], "replica", split_axis=1, concat_axis=0, tiled=True)
    mine_chosen = lax.dynamic_slice_in_dim(freq_rows, my_index * share, share, 1)
    band_update = decode(received, mine_chosen, basis).astype(jnp.bfloat16)
    update = lax.all_gather(band_update, "replica", axis=0, tiled=True)
    return (input_grad, momentum_out, update)


def fits(sizes, tokens, width, hidden):
    return (
        sizes["tensor"] == 4
        and sizes["replica"] == 8
        and tokens % 32 == 0
        and width == 2 * STEP
        and hidden % STRIP == 0
        and hidden <= STRIP * LANES
    )


def body(activations, grad_out, weight, momentum, freq_rows):
    sizes = {axis: lax.axis_size(axis) for axis in ("replica", "tensor")}
    fast = fits(sizes, *activations.shape, weight.shape[1])
    return (fast_body if fast else any_body)(activations, grad_out, weight, momentum, freq_rows)


def solution(mesh):
    placed = (
        P("replica", "tensor"),
        P("replica", "tensor"),
        P(None, "tensor"),
        P("replica", None, "tensor"),
        P(None, None, "tensor"),
    )
    return jax.shard_map(
        body,
        mesh=mesh,
        in_specs=placed,
        out_specs=(P("replica", "tensor"), P("replica", None, "tensor"), P(None, "tensor")),
        check_vma=False,
    )
```
